32 devices in a mesh: role: 2 (over core), ctx: 2 (over y), req: 8 (over z, x).
Axes of the slice: x: 2, y: 2, z: 4, core: 2. Of those that a mesh axis runs over, the one named last changes fastest.
Arguments:
- cache: bfloat16 [16, 8192, 576], P(None, ('ctx', 'req'), 'role'), may hold values from -8 to 8
- lengths: int32 [16], replicated, may hold values from 2 to 8192
- request_decode_slot: int32 [16], replicated, may hold values from 0 to 15, as said below
- q_nope: bfloat16 [16, 4, 16384], P('req', None, ('role', 'ctx')), may hold values from -6 to 6
- q_rope: bfloat16 [16, 4, 8192], P('req', None, ('role', 'ctx')), may hold values from -8 to 8
- new_latent: bfloat16 [16, 4, 576], P('req'), may hold values from -4.1875 to 4.1875
- w_key: bfloat16 [128, 128, 512], P(('role', 'ctx')), may hold values from -0.5 to 0.5
- value_up_weight: bfloat16 [128, 512, 128], P(('role', 'ctx')), may hold values from -1 to 1
Outputs:
- attended: bfloat16 [16, 4, 16384], P('req', None, ('role', 'ctx'))
The draws below stay inside these ranges and needn't reach their ends.
Inputs may be any that keep to these rules, and one draw needn't show every extreme that they name: A permutation of the slots; request r is owned by req index request_decode_slot[r] // 2.
All inputs are finite; a program needn't handle non-finite values.
Results may differ from the reference program's by a relative error of at most 0.007.
Values may be sent and summed in bfloat16 or wider, within the bound.
A program may use at most 128 MiB of HBM per device.

```python
import jax
import jax.numpy as jnp
from jax import lax

HEADS = 128
NOPE = 128
ROPE = 64
LATENT = 512
VDIM = 128
REQ_DEV = 2
BLOCK = 4096
STEPS = 4
REQS = 16
MAXLEN = 8192
N_CTX = 2
N_REQ = 8


def owner_table(key):
    return jax.random.permutation(jax.random.fold_in(key, 101), REQS).astype(jnp.int32)


def draw_request_decode_slot(key, part):
    return owner_table(key)


def draw_cache(key, part):
    base = jax.random.fold_in(key, 303)

    def one_request(index):
        first, second = jax.random.split(jax.random.fold_in(base, index))
        latent = jnp.clip(jax.random.normal(first, (MAXLEN, LATENT), jnp.float32) * 0.5, -3.0, 3.0)
        rotary = jnp.clip(jax.random.normal(second, (MAXLEN, ROPE), jnp.float32), -6.0, 6.0)
        return jnp.concatenate([latent, rotary], axis=1).astype(jnp.bfloat16)
    values = lax.map(one_request, jnp.arange(REQS, dtype=jnp.int32))
    return values


def draw_q_rope(key, part):
    values = jax.random.normal(jax.random.fold_in(key, 404), (REQS, STEPS, HEADS * ROPE), jnp.float32)
    values = jnp.clip(values, -6.0, 6.0)
    return values.astype(jnp.bfloat16)


def plant(drawn, stream_key, least, top_value):
    longest = drawn.shape.index(max(drawn.shape))
    spots = []
    for shift in (0, 1):
        where = [jax.random.randint(jax.random.fold_in(stream_key, axis), (), 0, length) for axis, length in enumerate(drawn.shape)]
        where[longest] = (where[longest] + shift) % drawn.shape[longest]
        spots.append(tuple(where))
    return drawn.at[spots[0]].set(least).at[spots[1]].set(top_value)


def shard_levels(key, dims, shards, least, largest):
    level = 1.0
    for position, shards_of in shards:
        draws = jax.random.uniform(jax.random.fold_in(jax.random.fold_in(key, 6), position), (shards_of,), jnp.float32, least / len(shards), largest / len(shards))
        level = level * jnp.repeat(jnp.exp(draws), dims[position] // shards_of).reshape((-1,) + (1,) * (len(dims) - 1 - position))
    return level


def noise(own_key, shape, deviation, reach, pieces=(), kind=jnp.bfloat16):
    gain = shard_levels(own_key, shape, pieces, -0.22, 0.18) if pieces else 1.0
    values = jax.random.normal(own_key, shape, jnp.float32) * deviation * gain
    return jnp.minimum(jnp.maximum(values, -reach), reach).astype(kind)


def setup_inputs(seed: int = 0) -> dict:
    key_of = jax.random.split(jax.random.key(seed), 9)
    return {
        "cache": draw_cache(jax.random.fold_in(key_of[8], 71), 0),
        "lengths": plant(jax.random.randint(key_of[1], (REQS,), 2, MAXLEN + 1), jax.random.fold_in(key_of[1], 1), 2, MAXLEN).astype(jnp.int32),
        "request_decode_slot": draw_request_decode_slot(jax.random.fold_in(key_of[8], 71), 0),
        "q_nope": noise(key_of[3], (REQS, STEPS, HEADS * NOPE), 1.0, 6.0, ((0, 8), (2, 4))),
        "q_rope": draw_q_rope(jax.random.fold_in(key_of[8], 71), 0),
        "new_latent": noise(key_of[5], (REQS, STEPS, LATENT + ROPE), 0.7, 4.1875, ((0, 8),)),
        "w_key": noise(key_of[6], (HEADS, NOPE, LATENT), NOPE ** -0.5, 0.5, ((0, 4),)),
        "value_up_weight": noise(key_of[7], (HEADS, LATENT, VDIM), (LATENT // 16) ** -0.5, 1.0, ((0, 4),)),
    }


def reference(cache, lengths, request_decode_slot, q_nope, q_rope, new_latent, w_key, value_up_weight):
    total_reqs = request_decode_slot.shape[0]
    inverse = jnp.zeros((total_reqs,), jnp.int32).at[request_decode_slot].set(jnp.arange(total_reqs, dtype=jnp.int32))
    softmax_scale = (NOPE + ROPE) ** -0.5
    key_weights = w_key.astype(jnp.float32)
    value_matrices = value_up_weight.astype(jnp.float32)
    step_ids = jnp.arange(STEPS, dtype=jnp.int32)
    causal = (step_ids[None, :] <= step_ids[:, None])[None, :, None, :]
    positions = jnp.arange(MAXLEN, dtype=jnp.int32)

    def one_owner(owner):
        first = (owner * REQ_DEV).astype(jnp.int32)
        requests = lax.dynamic_slice_in_dim(inverse, first, REQ_DEV)
        payload = cache[requests].astype(jnp.float32)
        visible = (positions[None, :] < lengths[requests][:, None])[:, None, None, :]
        queries = lax.dynamic_slice_in_dim(q_nope, first, REQ_DEV).astype(jnp.float32)
        queries = queries.reshape(REQ_DEV, STEPS, HEADS, NOPE)
        absorbed = jnp.einsum("gshd,hdk->gshk", queries, key_weights).astype(jnp.bfloat16)
        absorbed = lax.optimization_barrier(absorbed).astype(jnp.float32)
        rotary = lax.dynamic_slice_in_dim(q_rope, first, REQ_DEV).astype(jnp.float32)
        rotary = rotary.reshape(REQ_DEV, STEPS, HEADS, ROPE)
        query_rows = jnp.concatenate([absorbed, rotary], axis=3)
        fresh_rows = lax.dynamic_slice_in_dim(new_latent, first, REQ_DEV).astype(jnp.float32)
        scores = jnp.einsum("gshk,gpk->gshp", query_rows, payload) * softmax_scale
        fresh_scores = jnp.einsum("gshk,gtk->gsht", query_rows, fresh_rows) * softmax_scale
        highest = jnp.maximum(jnp.max(jnp.where(visible, scores, -1e30), axis=3),
                              jnp.max(jnp.where(causal, fresh_scores, -1e30), axis=3))
        weights = jnp.where(visible, jnp.exp(scores - highest[..., None]), 0.0)
        fresh_weights = jnp.where(causal, jnp.exp(fresh_scores - highest[..., None]), 0.0)
        normalizer = jnp.sum(weights, axis=3) + jnp.sum(fresh_weights, axis=3)
        rounded = lax.optimization_barrier(weights.astype(jnp.bfloat16)).astype(jnp.float32)
        rounded = rounded.reshape(REQ_DEV, STEPS, HEADS, N_CTX, BLOCK)
        fresh_rounded = lax.optimization_barrier(fresh_weights.astype(jnp.bfloat16)).astype(jnp.float32)
        latent_rows = payload[:, :, :LATENT].reshape(REQ_DEV, N_CTX, BLOCK, LATENT)
        partials = jnp.einsum("gshcp,gcpk->gshck", rounded, latent_rows)
        fresh_part = jnp.einsum("gsht,gtk->gshk", fresh_rounded, fresh_rows[:, :, :LATENT])
        partials = partials.at[:, :, :, 0].add(fresh_part)
        partials = lax.optimization_barrier(partials.astype(jnp.bfloat16)).astype(jnp.float32)
        numerators = jnp.sum(partials, axis=3)
        combined_result = (numerators / normalizer[..., None]).astype(jnp.bfloat16)
        combined_result = lax.optimization_barrier(combined_result).astype(jnp.float32)
        output_rows = jnp.einsum("jnay,ayp->jnap", combined_result, value_matrices).astype(jnp.bfloat16)
        return output_rows.reshape(REQ_DEV, STEPS, HEADS * VDIM)

    stacked = lax.map(one_owner, jnp.arange(N_REQ, dtype=jnp.int32))
    return stacked.reshape(total_reqs, STEPS, HEADS * VDIM)
```

```python
import functools
import math

import jax
import jax.numpy as jnp
from jax import lax
from jax.experimental import pallas as pl
from jax.experimental.pallas import tpu as pltpu
from jax.sharding import PartitionSpec as P

NEG = -1e30
LOW = -1e29
MESH = pl.DeviceIdType.MESH
BLOCK_HEADS = 4


def xor_bit(value, bit, flip):
    b = lax.rem(lax.div(value, bit), 2)
    return value + flip * bit * (1 - 2 * b)


def owner_of(cl, k, chip):
    if cl == 0:
        return lax.rem(chip, 4) + 4 * k
    if cl == 1:
        return lax.rem(chip, 2) + 2 * lax.rem(k, 2) + 8 * lax.div(k, 2)
    return lax.rem(k, 2) + 2 * lax.rem(lax.div(chip, 2), 2) + 4 + 8 * lax.div(k, 2)


def neighbour(cl, p, chip):
    if cl == 0:
        return xor_bit(xor_bit(chip, 1, p % 2), 2, p // 2)
    return xor_bit(chip, cl, p)


def kernel(dims, inv_ref, len_ref, cache_ref, qn_ref, qr_ref, new_ref, wk_ref, vu_ref, out_ref,
           cache_v, ksend, k_a, k_b, wk_v, vu_v, rawn, rawr, qa, q_in, r_in, s_buf, m_buf, l_buf, acc,
           o_out, e_out, o_in, e_in, merged, att_out, f_out, att_a, f_a, att_b, f_b,
           load_sem, raw_ss, raw_rs, k_ss, ka_rs, kb_rs, q_ss, q_rs, o_ss, o_rs, t_ss, ta_rs, tb_rs):
    n_req, n_ctx, steps, scale2 = dims
    role, ctx, req = lax.axis_index("role"), lax.axis_index("ctx"), lax.axis_index("req")
    per = n_req // 8
    two = 2 * per
    high = n_req // 4
    total, half, span = cache_ref.shape
    heads, nope, latent = wk_ref.shape
    rows = heads * steps
    low, hi = lax.rem(req, 4), lax.div(req, 4)
    bit2 = lax.rem(hi, 2)
    other = 1 - role

    def role_at(rr):
        return role if rr == 0 else other

    def ctx_at(t):
        return lax.rem(ctx + t, n_ctx)

    loads = [pltpu.make_async_copy(cache_ref, cache_v, load_sem.at[0]),
             pltpu.make_async_copy(wk_ref, wk_v, load_sem.at[1]),
             pltpu.make_async_copy(vu_ref, vu_v, load_sem.at[2])]
    loads[0].start()
    loads[1].start()

    partners = []
    for d in (1, 2, 3):
        for rr in (0, 1):
            partners.append((role_at(rr), ctx, neighbour(0, d, req)))
    for t in range(n_ctx):
        for rr in (0, 1):
            if t or rr:
                partners.append((role_at(rr), ctx_at(t), req))
    for v in range(1, high):
        far = 4 * lax.rem(hi + v, high)
        for d in (0, 1, 2):
            partners.append((role, ctx, neighbour(0, d, low) + far))
    barrier = pltpu.get_barrier_semaphore()
    for dev in partners:
        pl.semaphore_signal(barrier, inc=1, device_id=dev, device_id_type=MESH)
    pl.semaphore_wait(barrier, len(partners))

    started = []

    def send(src, dst, ss, rs, dev):
        copy = pltpu.make_async_remote_copy(src_ref=src, dst_ref=dst, send_sem=ss, recv_sem=rs, device_id=dev,
                                            device_id_type=MESH)
        copy.start()
        started.append(copy)

    def arrived(ref, sem):
        pltpu.make_async_copy(ref, ref, sem).wait()

    mine_b = (1 + bit2) * two + lax.rem(lax.div(req, 2 - bit2), 2) * 0
    kk = jnp.where(bit2 == 0, lax.rem(lax.div(req, 2), 2), lax.rem(req, 2)) + 2 * lax.div(req, 8)
    mine_b = (1 + bit2) * two + kk
    mine_a = hi
    low_b = jnp.where(bit2 == 0, xor_bit(low, 2, 1), xor_bit(low, 1, 1))
    index = 0
    for slot, spot, dests in (
        (1, mine_b, [(u, v) for v in range(high) for u in (0, 1) if u or v]),
        (0, mine_a, [(0, v) for v in range(1, high)]),
    ):
        for u, v in dests:
            chip = (low_b if u else low) + 4 * lax.rem(hi + v, high)
            dev = (role, ctx, chip)
            send(qn_ref.at[slot], rawn.at[spot], raw_ss.at[index, 0], raw_rs.at[spot, 0], dev)
            send(qr_ref.at[slot], rawr.at[spot], raw_ss.at[index, 1], raw_rs.at[spot, 1], dev)
            index += 1
        rawn[spot] = qn_ref[slot]
        rawr[spot] = qr_ref[slot]

    loads[0].wait()
    loads[2].start()

    def k_ref(cl, m, p):
        return k_a.at[m, p] if cl == 0 else k_b.at[(cl - 1) * per + m, p]

    def k_sem(cl, m, p, h):
        return ka_rs.at[m, p, h] if cl == 0 else kb_rs.at[(cl - 1) * per + m, p, h]

    mine_rows = pl.ds(pl.multiple_of(role * half, 16), half)
    sends = []
    order = [(1, 1), (2, 1), (1, 0), (2, 0), (0, 1), (0, 2), (0, 3), (0, 0)]
    for cl, p in order:
        for rr in (0, 1):
            for m in range(per):
                sends.append((cl, p, rr, m))
    pending = None
    chunk = 0
    for cl, p, rr, m in sends:
        chip = neighbour(cl, p, req)
        slot = 2 * owner_of(cl, 2 * m + role_at(rr), chip) + (1 if cl else 0)
        data = cache_v[inv_ref[slot]]
        dst = k_ref(cl, m, p)
        if p == 0 and rr == 0:
            dst[mine_rows, :] = data
            continue
        ksend[chunk] = data
        if pending is not None:
            send(*pending)
        pending = (ksend.at[chunk], dst.at[mine_rows, :], k_ss.at[chunk], k_sem(cl, m, p, role),
                   (role_at(rr), ctx, chip))
        chunk += 1
    send(*pending)

    loads[1].wait()
    block = BLOCK_HEADS * steps
    lhs_rows = lax.broadcasted_iota(jnp.int32, (two * block, BLOCK_HEADS * nope), 0)
    lhs_cols = lax.broadcasted_iota(jnp.int32, (two * block, BLOCK_HEADS * nope), 1)
    diagonal = (lax.div(lax.rem(lhs_rows, block), steps) == lax.div(lhs_cols, nope)).astype(jnp.float32)
    diagonal = diagonal.astype(jnp.bfloat16)

    qcount = 0
    for cl in (1, 2, 0):
        for k in range(two):
            @pl.when(owner_of(cl, jnp.int32(k), req) != req)
            def _():
                arrived(rawn.at[cl * two + k], raw_rs.at[cl * two + k, 0])
                arrived(rawr.at[cl * two + k], raw_rs.at[cl * two + k, 1])

        def absorb(hb, carry):
            r0 = pl.multiple_of(hb * block, block)
            lhs = jnp.concatenate([rawn[cl * two + k, pl.ds(r0, block), :] for k in range(two)], axis=0)
            lhs = jnp.concatenate([lhs] * BLOCK_HEADS, axis=1) * diagonal
            w = wk_v[pl.ds(hb * BLOCK_HEADS, BLOCK_HEADS)].reshape(BLOCK_HEADS * nope, latent)
            res = jnp.dot(lhs, w, preferred_element_type=jnp.float32).astype(jnp.bfloat16)
            for k in range(two):
                qa[cl * two + k, pl.ds(r0, block), :] = res[k * block:(k + 1) * block]
            return carry

        lax.fori_loop(0, heads // BLOCK_HEADS, absorb, 0)
        for t in list(range(1, n_ctx)) + [0]:
            for rr in (0, 1):
                for m in range(per):
                    if t == 0 and rr == 0:
                        continue
                    k = cl * two + 2 * m + role_at(rr)
                    at = ((n_ctx - t) % n_ctx) * 2 + rr
                    dev = (role_at(rr), ctx_at(t), req)
                    send(rawr.at[k], r_in.at[cl * per + m, at], q_ss.at[qcount, 1], q_rs.at[cl * per + m, at, 1], dev)
                    send(qa.at[k], q_in.at[cl * per + m, at], q_ss.at[qcount, 0], q_rs.at[cl * per + m, at, 0], dev)
                    qcount += 1

    ocount = 0
    for cl in (1, 2, 0):
        parts = 4 if cl == 0 else 2
        for m in range(per):
            sl = cl * per + m
            owner = owner_of(cl, 2 * m + role, req)
            slot = 2 * owner + (1 if cl else 0)
            length = len_ref[inv_ref[slot]]
            fresh_on = jnp.logical_and(owner == req, ctx == 0)
            for nth, rel in enumerate(list(range(1, n_ctx)) + [0]):
                for rr in (0, 1):
                    if rel or rr:
                        arrived(q_in.at[sl, rel * 2 + rr], q_rs.at[sl, rel * 2 + rr, 0])
                        arrived(r_in.at[sl, rel * 2 + rr], q_rs.at[sl, rel * 2 + rr, 1])
                if rel == 0:
                    q_own, r_own = qa[cl * two + 2 * m + role], rawr[cl * two + 2 * m + role]
                else:
                    q_own, r_own = q_in[sl, rel * 2], r_in[sl, rel * 2]
                q = jnp.concatenate([q_own, q_in[sl, rel * 2 + 1]], axis=0)
                qr = jnp.concatenate([r_own.astype(jnp.float32).T, r_in[sl, rel * 2 + 1].astype(jnp.float32).T],
                                     axis=0).astype(jnp.bfloat16)
                new = new_ref[1 if cl else 0]
                nt = (((1,), (1,)), ((), ()))
                fresh = (lax.dot_general(q, new[:, :latent], nt, preferred_element_type=jnp.float32)
                         + lax.dot_general(qr, new[:, latent:], nt, preferred_element_type=jnp.float32)) * scale2
                token = lax.broadcasted_iota(jnp.int32, fresh.shape, 1)
                step = lax.rem(lax.broadcasted_iota(jnp.int32, fresh.shape, 0), steps)
                last = jnp.where(fresh_on, step, -1)
                fresh = jnp.where(token <= last, fresh, NEG)
                m_buf[...] = jnp.broadcast_to(jnp.max(fresh, axis=1, keepdims=True), m_buf.shape)

                def score(p, carry):
                    if nth == 0:
                        @pl.when(p > 0)
                        def _():
                            arrived(k_ref(cl, m, 0).at[pl.ds(0, half), :], k_sem(cl, m, p, role))
                        arrived(k_ref(cl, m, 0).at[pl.ds(0, half), :], k_sem(cl, m, p, other))
                    kk_ = k_ref(cl, m, p)
                    s = jnp.dot(q, kk_[:latent, :], preferred_element_type=jnp.float32)
                    s += jnp.dot(qr, kk_[latent:, :], preferred_element_type=jnp.float32)
                    if cl == 0:
                        chip = xor_bit(xor_bit(req, 1, lax.rem(p, 2)), 2, lax.div(p, 2))
                    else:
                        chip = xor_bit(req, cl, p)
                    first = (ctx * n_req + chip) * span
                    position = first + lax.broadcasted_iota(jnp.int32, (1, span), 1)
                    s = jnp.where(position < length, s * scale2, NEG)
                    s_buf[p] = s
                    m_buf[...] = jnp.maximum(m_buf[...], jnp.max(s, axis=1, keepdims=True))
                    return carry

                lax.fori_loop(0, parts, score, 0)
                top = jnp.maximum(m_buf[:, :1], LOW)
                weights = jnp.exp2(fresh - top)
                l_buf[...] = jnp.broadcast_to(jnp.sum(weights, axis=1, keepdims=True), l_buf.shape)
                acc[...] = jnp.dot(weights.astype(jnp.bfloat16), new[:, :latent], preferred_element_type=jnp.float32)

                def weigh(p, carry):
                    w = jnp.exp2(s_buf[p] - jnp.maximum(m_buf[:, :1], LOW))
                    l_buf[...] += jnp.sum(w, axis=1, keepdims=True)
                    acc[...] += lax.dot_general(w.astype(jnp.bfloat16), k_ref(cl, m, p)[:latent, :], nt,
                                                preferred_element_type=jnp.float32)
                    return carry

                lax.fori_loop(0, parts, weigh, 0)
                norm = l_buf[:, :1]
                live = norm > 0.0
                safe = jnp.where(live, norm, 1.0)
                o = (acc[...] * (1.0 / safe)).astype(jnp.bfloat16)
                lse = jnp.where(live, top + jnp.log2(safe), NEG)
                lse = jnp.broadcast_to(lse, (2 * rows, 128))
                k = cl * two + 2 * m + role
                back = (n_ctx - rel) % n_ctx
                for rr in (0, 1):
                    piece = o[rr * rows:(rr + 1) * rows]
                    e = lse[rr * rows:(rr + 1) * rows].T[:8]
                    if rel == 0 and rr == 0:
                        o_in[k, 0] = piece
                        e_in[k, 0] = e
                        continue
                    o_out[sl, rel * 2 + rr] = piece
                    e_out[sl, rel * 2 + rr] = e
                    dev = (role_at(rr), ctx_at(rel), req)
                    send(e_out.at[sl, rel * 2 + rr], e_in.at[k, back], o_ss.at[ocount, 1], o_rs.at[k, back, 1], dev)
                    send(o_out.at[sl, rel * 2 + rr], o_in.at[k, back], o_ss.at[ocount, 0], o_rs.at[k, back, 0], dev)
                    ocount += 1

    loads[2].wait()
    out_rows = lax.broadcasted_iota(jnp.int32, (two * block, 128), 0)
    which = lax.div(lax.rem(out_rows, block), steps)
    guarded = []
    for cl in (1, 2, 0):
        for rr in (0, 1):
            for m in range(per):
                k = cl * two + 2 * m + role_at(rr)
                for rel in range(n_ctx):
                    if rr or rel:
                        arrived(o_in.at[k, rel], o_rs.at[k, rel, 0])
                        arrived(e_in.at[k, rel], o_rs.at[k, rel, 1])
                es = [e_in[k, rel] for rel in range(n_ctx)]
                top = functools.reduce(jnp.maximum, es)
                shares = [jnp.exp2(e - top) for e in es]
                norm = sum(shares)
                f_out[k] = top + jnp.log2(norm)
                value = 0.0
                for rel in range(n_ctx):
                    w = jnp.broadcast_to((shares[rel] / norm)[:1], (128, rows)).T
                    w = jnp.concatenate([w] * (latent // 128), axis=1)
                    value = value + o_in[k, rel].astype(jnp.float32) * w
                merged[k] = value.astype(jnp.bfloat16)

        def up(hb, carry):
            r0 = pl.multiple_of(hb * block, block)
            lhs = jnp.concatenate([merged[cl * two + k, pl.ds(r0, block), :] for k in range(two)], axis=0)
            res = jnp.zeros((two * block, 128), jnp.float32)
            for j in range(BLOCK_HEADS):
                one = jnp.dot(lhs, vu_v[hb * BLOCK_HEADS + j], preferred_element_type=jnp.float32)
                res = jnp.where(which == j, one, res)
            res = res.astype(jnp.bfloat16)
            for k in range(two):
                att_out[cl * two + k, pl.ds(r0, block), :] = res[k * block:(k + 1) * block]
            return carry

        lax.fori_loop(0, heads // BLOCK_HEADS, up, 0)
        for k in range(two):
            e = cl * two + k
            owner = owner_of(cl, jnp.int32(k), req)
            if cl == 0:
                at, dst, fdst, sems = hi, att_a, f_a, ta_rs
            elif cl == 1:
                at, dst, fdst, sems = lax.div(req, 2), att_b, f_b, tb_rs
            else:
                at, dst, fdst, sems = lax.rem(req, 2) + 2 * hi, att_b, f_b, tb_rs
            copies = [
                pltpu.make_async_remote_copy(
                    src_ref=src.at[e], dst_ref=d.at[at], send_sem=t_ss.at[e, j], recv_sem=sems.at[at, j],
                    device_id=(role, ctx, owner), device_id_type=MESH)
                for j, (src, d) in enumerate(((att_out, dst), (f_out, fdst)))
            ]

            @pl.when(owner != req)
            def _():
                for copy in copies:
                    copy.start()

            @pl.when(owner == req)
            def _():
                dst[at] = att_out[e]
                fdst[at] = f_out[e]
            guarded.append((owner, copies))

    own_b = jnp.where(bit2 == 0, lax.div(req, 2), lax.rem(req, 2) + 2 * hi)
    for slot, count, src, fsrc, sems, own in ((1, 4 * per, att_b, f_b, tb_rs, own_b), (0, high, att_a, f_a, ta_rs, hi)):
        for j in range(count):
            @pl.when(own != j)
            def _():
                arrived(src.at[j], sems.at[j, 0])
                arrived(fsrc.at[j], sems.at[j, 1])
        es = [fsrc[j] for j in range(count)]
        top = functools.reduce(jnp.maximum, es)
        shares = [jnp.exp2(e - top) for e in es]
        norm = sum(shares)
        value = 0.0
        for j in range(count):
            w = jnp.broadcast_to((shares[j] / norm)[:1], (128, rows)).T
            value = value + src[j].astype(jnp.float32) * w
        out_ref[slot] = value.astype(jnp.bfloat16)

    for copy in started:
        copy.wait_send()
    for owner, copies in guarded:
        @pl.when(owner != req)
        def _():
            for copy in copies:
                copy.wait_send()


def shards(cache, lengths, request_decode_slot, q_nope, q_rope, new_latent, w_key, value_up_weight):
    total = request_decode_slot.shape[0]
    n_req, n_ctx = lax.axis_size("req"), lax.axis_size("ctx")
    heads, nope, latent = w_key.shape
    vdim = value_up_weight.shape[2]
    own, steps = q_nope.shape[:2]
    rope = q_rope.shape[2] // heads
    span, half = cache.shape[1:]
    rows = heads * steps
    per, two, high = n_req // 8, n_req // 4, n_req // 4
    groups = 2 * n_ctx
    scale2 = (nope + rope) ** (-0.5) * math.log2(math.e)

    slots = jnp.arange(total, dtype=jnp.int32)
    inverse = jnp.sum(
        jnp.where(request_decode_slot[None, :] == slots[:, None], slots[None, :], 0), axis=1
    ).astype(jnp.int32)
    turned = jnp.swapaxes(cache, 1, 2)
    qn = q_nope.reshape(own, steps, heads, nope).swapaxes(1, 2).reshape(own, rows, nope)
    qr = q_rope.reshape(own, steps, heads, rope).transpose(0, 3, 2, 1).reshape(own, rope, rows)
    new = jnp.pad(new_latent, ((0, 0), (0, 128 - steps), (0, 0)))
    bf, f32 = jnp.bfloat16, jnp.float32
    chunks = total - 3 * per
    vm, dma = pltpu.VMEM, pltpu.SemaphoreType.DMA
    smem = pl.BlockSpec(memory_space=pltpu.SMEM)
    here = pl.BlockSpec(memory_space=pltpu.VMEM)
    away = pl.BlockSpec(memory_space=pl.ANY)
    out = pl.pallas_call(
        functools.partial(kernel, (n_req, n_ctx, steps, scale2)),
        out_shape=jax.ShapeDtypeStruct((own, rows, vdim), bf),
        in_specs=[smem, smem, away, here, here, here, away, away],
        out_specs=here,
        scratch_shapes=[
            vm((total, half, span), bf),
            vm((chunks, half, span), bf),
            vm((per, 4, 2 * half, span), bf),
            vm((2 * per, 2, 2 * half, span), bf),
            vm(w_key.shape, bf),
            vm(value_up_weight.shape, bf),
            vm((3 * two, rows, nope), bf),
            vm((3 * two, rope, rows), bf),
            vm((3 * two, rows, latent), bf),
            vm((3 * per, groups, rows, latent), bf),
            vm((3 * per, groups, rope, rows), bf),
            vm((4, 2 * rows, span), f32),
            vm((2 * rows, 128), f32),
            vm((2 * rows, 128), f32),
            vm((2 * rows, latent), f32),
            vm((3 * per, groups, rows, latent), bf),
            vm((3 * per, groups, 8, rows), f32),
            vm((3 * two, n_ctx, rows, latent), bf),
            vm((3 * two, n_ctx, 8, rows), f32),
            vm((3 * two, rows, latent), bf),
            vm((3 * two, rows, vdim), bf),
            vm((3 * two, 8, rows), f32),
            vm((high, rows, vdim), bf),
            vm((high, 8, rows), f32),
            vm((4 * per, rows, vdim), bf),
            vm((4 * per, 8, rows), f32),
            dma((3,)),
            dma((3 * high, 2)),
            dma((3 * two, 2)),
            dma((chunks,)),
            dma((per, 4, 2)),
            dma((2 * per, 2, 2)),
            dma((3 * per * (groups - 1), 2)),
            dma((3 * per, groups, 2)),
            dma((3 * per * (groups - 1), 2)),
            dma((3 * two, n_ctx, 2)),
            dma((3 * two, 2)),
            dma((high, 2)),
            dma((4 * per, 2)),
        ],
        compiler_params=pltpu.CompilerParams(
            collective_id=0, has_side_effects=True, vmem_limit_bytes=62 * 1024 * 1024
        ),
    )(inverse, lengths, turned, qn, qr, new, w_key, value_up_weight)
    return out.reshape(own, heads, steps, vdim).swapaxes(1, 2).reshape(own, steps, heads * vdim)


def solution(mesh):
    placed = (
        P(None, ("ctx", "req"), "role"),
        P(),
        P(),
        P("req", None, ("role", "ctx")),
        P("req", None, ("role", "ctx")),
        P("req", None, None),
        P(("role", "ctx"), None, None),
        P(("role", "ctx"), None, None),
    )
    return jax.shard_map(
        shards,
        mesh=mesh,
        in_specs=placed,
        out_specs=P("req", None, ("role", "ctx")),
        check_vma=False,
    )
```

```python
import functools
import math

import jax
import jax.numpy as jnp
from jax import lax
from jax.experimental import pallas as pl
from jax.experimental.pallas import tpu as pltpu
from jax.sharding import PartitionSpec as P

NEG = -1e30
LOW = -1e29
MESH = pl.DeviceIdType.MESH
BLOCK_HEADS = 4


def xor_bit(value, bit, flip):
    b = lax.rem(lax.div(value, bit), 2)
    return value + flip * bit * (1 - 2 * b)


def owner_of(cl, k, chip):
    if cl == 0:
        return lax.rem(chip, 4) + 4 * k
    if cl == 1:
        return lax.rem(chip, 2) + 2 * lax.rem(k, 2) + 8 * lax.div(k, 2)
    return lax.rem(k, 2) + 2 * lax.rem(lax.div(chip, 2), 2) + 4 + 8 * lax.div(k, 2)


def neighbour(cl, p, chip):
    if cl == 0:
        return xor_bit(xor_bit(chip, 1, p % 2), 2, p // 2)
    return xor_bit(chip, cl, p)


def kernel(dims, slot_ref, len_ref, cache_ref, qn_ref, qr_ref, new_ref, wk_ref, vu_ref, out_ref,
           cache_v, ksend, k_a, k_b, wk_v, vu_v, qn_f, qr_f, qn_s, qr_s, new_f, rawn, rawr, qa, q_in, r_in,
           m_st, l_st, acc, o_out, e_out, o_in, e_in, merged, att_out, f_out, att_a, f_a, att_b, f_b, fin,
           load_sem, raw_ss, raw_rs, k_ss, ka_rs, kb_rs, q_ss, q_rs, o_ss, o_rs, t_ss, ta_rs, tb_rs):
    n_req, n_ctx, scale2 = dims
    role, ctx, req = lax.axis_index("role"), lax.axis_index("ctx"), lax.axis_index("req")
    per = n_req // 8
    two = 2 * per
    high = n_req // 4
    total, half, span = cache_ref.shape
    heads, nope, latent = wk_ref.shape
    own, steps = qn_ref.shape[:2]
    rows = heads * steps
    pairs = heads // 2
    low, hi = lax.rem(req, 4), lax.div(req, 4)
    bit2 = lax.rem(hi, 2)
    other = 1 - role

    def role_at(rr):
        return role if rr == 0 else other

    def ctx_at(t):
        return lax.rem(ctx + t, n_ctx)

    loads = [pltpu.make_async_copy(cache_ref, cache_v, load_sem.at[0]),
             pltpu.make_async_copy(wk_ref, wk_v, load_sem.at[1]),
             pltpu.make_async_copy(vu_ref, vu_v, load_sem.at[2])]
    loads[0].start()
    loads[1].start()

    partners = []
    for d in (1, 2, 3):
        for rr in (0, 1):
            partners.append((role_at(rr), ctx, neighbour(0, d, req)))
    for t in range(n_ctx):
        for rr in (0, 1):
            if t or rr:
                partners.append((role_at(rr), ctx_at(t), req))
    for v in range(1, high):
        far = 4 * lax.rem(hi + v, high)
        for d in (0, 1, 2):
            partners.append((role, ctx, neighbour(0, d, low) + far))
    barrier = pltpu.get_barrier_semaphore()
    for dev in partners:
        pl.semaphore_signal(barrier, inc=1, device_id=dev, device_id_type=MESH)

    started = []

    def send(src, dst, ss, rs, dev):
        copy = pltpu.make_async_remote_copy(src_ref=src, dst_ref=dst, send_sem=ss, recv_sem=rs, device_id=dev,
                                            device_id_type=MESH)
        copy.start()
        started.append(copy)

    def arrived(ref, sem):
        pltpu.make_async_copy(ref, ref, sem).wait()

    def first_row(h):
        return ((h % 2) * pairs + h // 2) * steps

    for slot in range(own):
        for h in range(heads):
            r = first_row(h)
            qn_f[slot, r:r + steps, :] = qn_ref[slot, :, h * nope:(h + 1) * nope].astype(jnp.float32)
        for h in range(pairs):
            qr_f[slot, h * steps:(h + 1) * steps, :] = qr_ref[slot, :, h * 128:(h + 1) * 128].astype(jnp.float32)
        qn_s[slot] = qn_f[slot].astype(jnp.bfloat16)
        qr_s[slot] = qr_f[slot].astype(jnp.bfloat16)
    new_f[...] = jnp.zeros_like(new_f)
    for slot in range(own):
        fresh_rows = new_ref[slot].astype(jnp.float32)
        new_f[slot, :steps, :latent] = fresh_rows[:, :latent]
        new_f[slot, :steps, latent:] = jnp.concatenate([fresh_rows[:, latent:]] * 2, axis=1)

    def request_of(slot):
        def body(j, acc_):
            return jnp.where(slot_ref[j] == slot, j, acc_)
        if total <= 16:
            r = jnp.int32(0)
            for j in range(total):
                r = body(j, r)
            return r
        return lax.fori_loop(0, total, body, jnp.int32(0))

    def k_ref(cl, m, p):
        return k_a.at[m, p] if cl == 0 else k_b.at[(cl - 1) * per + m, p]

    def k_sem(cl, m, p, h):
        return ka_rs.at[m, p, h] if cl == 0 else kb_rs.at[(cl - 1) * per + m, p, h]

    mine_rows = pl.ds(pl.multiple_of(role * half, 16), half)
    order = [(1, 1), (2, 1), (1, 0), (2, 0), (0, 1), (0, 2), (0, 3), (0, 0)]
    todo, lengths = [], {}
    for cl, p in order:
        for rr in (0, 1):
            for m in range(per):
                chip = neighbour(cl, p, req)
                slot = 2 * owner_of(cl, 2 * m + role_at(rr), chip) + (1 if cl else 0)
                todo.append((cl, p, rr, m, chip, request_of(slot)))
    loads[0].wait()
    loads[2].start()
    pending = []
    chunk = 0
    for cl, p, rr, m, chip, request in todo:
        dst = k_ref(cl, m, p)
        if p == 0 and rr == 0:
            dst[mine_rows, :] = cache_v[request]
            lengths[cl, m] = len_ref[request]
            continue
        ksend[chunk] = cache_v[request]
        pending.append((ksend.at[chunk], dst.at[mine_rows, :], k_ss.at[chunk], k_sem(cl, m, p, role),
                        (role_at(rr), ctx, chip)))
        chunk += 1

    kk = jnp.where(bit2 == 0, lax.rem(lax.div(req, 2), 2), lax.rem(req, 2)) + 2 * lax.div(req, 8)
    low_b = jnp.where(bit2 == 0, xor_bit(low, 2, 1), xor_bit(low, 1, 1))
    raws = ((1, (1 + bit2) * two + kk, [(u, v) for v in range(high) for u in (0, 1) if u or v]),
            (0, hi, [(0, v) for v in range(1, high)]))
    for slot, spot, dests in raws:
        rawn[spot] = qn_s[slot]
        rawr[spot] = qr_s[slot]

    pl.semaphore_wait(barrier, len(partners))

    index = 0
    for slot, spot, dests in raws:
        for u, v in dests:
            chip = (low_b if u else low) + 4 * lax.rem(hi + v, high)
            dev = (role, ctx, chip)
            send(qn_s.at[slot], rawn.at[spot], raw_ss.at[index, 0], raw_rs.at[spot, 0], dev)
            send(qr_s.at[slot], rawr.at[spot], raw_ss.at[index, 1], raw_rs.at[spot, 1], dev)
            index += 1
    for one in pending:
        send(*one)

    loads[1].wait()
    block = BLOCK_HEADS * steps
    half_blocks = pairs // BLOCK_HEADS
    lhs_rows = lax.broadcasted_iota(jnp.int32, (two * block, BLOCK_HEADS * nope), 0)
    lhs_cols = lax.broadcasted_iota(jnp.int32, (two * block, BLOCK_HEADS * nope), 1)
    diagonal = (lax.div(lax.rem(lhs_rows, block), steps) == lax.div(lhs_cols, nope)).astype(jnp.float32)
    diagonal = diagonal.astype(jnp.bfloat16)

    def head_at(hb, j):
        return 2 * (BLOCK_HEADS * lax.rem(hb, half_blocks) + j) + lax.div(hb, half_blocks)

    qcount = 0
    for cl in (1, 2, 0):
        for k in range(two):
            @pl.when(owner_of(cl, jnp.int32(k), req) != req)
            def _():
                arrived(rawn.at[cl * two + k], raw_rs.at[cl * two + k, 0])
                arrived(rawr.at[cl * two + k], raw_rs.at[cl * two + k, 1])

        def absorb(hb, carry):
            r0 = pl.multiple_of(hb * block, block)
            lhs = jnp.concatenate([rawn[cl * two + k, pl.ds(r0, block), :] for k in range(two)], axis=0)
            lhs = jnp.concatenate([lhs] * BLOCK_HEADS, axis=1) * diagonal
            w = jnp.concatenate([wk_v[head_at(hb, j)] for j in range(BLOCK_HEADS)], axis=0)
            res = jnp.dot(lhs, w, preferred_element_type=jnp.float32).astype(jnp.bfloat16)
            for k in range(two):
                qa[cl * two + k, pl.ds(r0, block), :] = res[k * block:(k + 1) * block]
            return carry

        lax.fori_loop(0, heads // BLOCK_HEADS, absorb, 0)
        for t in list(range(1, n_ctx)) + [0]:
            for rr in (0, 1):
                for m in range(per):
                    if t == 0 and rr == 0:
                        continue
                    k = cl * two + 2 * m + role_at(rr)
                    at = ((n_ctx - t) % n_ctx) * 2 + rr
                    dev = (role_at(rr), ctx_at(t), req)
                    send(rawr.at[k], r_in.at[cl * per + m, at], q_ss.at[qcount, 1], q_rs.at[cl * per + m, at, 1], dev)
                    send(qa.at[k], q_in.at[cl * per + m, at], q_ss.at[qcount, 0], q_rs.at[cl * per + m, at, 0], dev)
                    qcount += 1

    nt = (((1,), (1,)), ((), ()))
    rels = list(range(1, n_ctx)) + [0]
    lane = lax.broadcasted_iota(jnp.int32, (rows // 2, 128), 1)
    even = (lane < 64).astype(jnp.float32).astype(jnp.bfloat16)
    odd = (lane >= 64).astype(jnp.float32).astype(jnp.bfloat16)

    def queries(cl, m, rel):
        sl, k = cl * per + m, cl * two + 2 * m + role
        if rel == 0:
            q_own, r_own = qa[k], rawr[k]
        else:
            q_own, r_own = q_in[sl, rel * 2], r_in[sl, rel * 2]
        r_far = r_in[sl, rel * 2 + 1]
        q = jnp.concatenate([q_own, q_in[sl, rel * 2 + 1]], axis=0)
        qr = jnp.concatenate([r_own * even, r_own * odd, r_far * even, r_far * odd], axis=0)
        return q, qr

    def open_slot(cl, m):
        sl = cl * per + m
        fresh_on = jnp.logical_and(owner_of(cl, 2 * m + role, req) == req, ctx == 0)
        new = new_f[1 if cl else 0].astype(jnp.bfloat16)
        for nth, rel in enumerate(rels):
            for rr in (0, 1):
                if rel or rr:
                    arrived(q_in.at[sl, rel * 2 + rr], q_rs.at[sl, rel * 2 + rr, 0])
                    arrived(r_in.at[sl, rel * 2 + rr], q_rs.at[sl, rel * 2 + rr, 1])
            q, qr = queries(cl, m, rel)
            fresh = (lax.dot_general(q, new[:, :latent], nt, preferred_element_type=jnp.float32)
                     + lax.dot_general(qr, new[:, latent:], nt, preferred_element_type=jnp.float32)) * scale2
            token = lax.broadcasted_iota(jnp.int32, fresh.shape, 1)
            step = lax.rem(lax.broadcasted_iota(jnp.int32, fresh.shape, 0), steps)
            fresh = jnp.where(token <= jnp.where(fresh_on, step, -1), fresh, NEG)
            top = jnp.maximum(jnp.max(fresh, axis=1, keepdims=True), LOW)
            weights = jnp.exp2(fresh - top)
            m_st[nth] = jnp.broadcast_to(top, (2 * rows, 128))
            l_st[nth] = jnp.broadcast_to(jnp.sum(weights, axis=1, keepdims=True), (2 * rows, 128))
            acc[nth] = jnp.dot(weights.astype(jnp.bfloat16), new[:, :latent], preferred_element_type=jnp.float32)

    def await_part(cl, m, p):
        sample = k_ref(cl, m, 0).at[pl.ds(0, half), :]

        @pl.when(p > 0)
        def _():
            arrived(sample, k_sem(cl, m, p, role))
        arrived(sample, k_sem(cl, m, p, other))

    def part(cl, m, p, nth):
        q, qr = queries(cl, m, rels[nth])
        keys = k_ref(cl, m, p)
        rotary = keys[latent:, :]
        s = jnp.dot(q, keys[:latent, :], preferred_element_type=jnp.float32)
        s += jnp.dot(qr, jnp.concatenate([rotary, rotary], axis=0), preferred_element_type=jnp.float32)
        if cl == 0:
            chip = xor_bit(xor_bit(req, 1, lax.rem(p, 2)), 2, lax.div(p, 2))
        else:
            chip = xor_bit(req, cl, p)
        position = (ctx * n_req + chip) * span + lax.broadcasted_iota(jnp.int32, (1, span), 1)
        s = jnp.where(position < lengths[cl, m], s * scale2, NEG)
        before = m_st[nth][:, :1]
        top = jnp.maximum(before, jnp.max(s, axis=1, keepdims=True))
        keep = jnp.exp2(before - top)
        w = jnp.exp2(s - top)
        m_st[nth] = jnp.broadcast_to(top, (2 * rows, 128))
        l_st[nth] = l_st[nth] * keep + jnp.sum(w, axis=1, keepdims=True)
        acc[nth] = acc[nth] * keep + lax.dot_general(w.astype(jnp.bfloat16), keys[:latent, :], nt,
                                                     preferred_element_type=jnp.float32)

    ocount = [0]

    def close_block(cl, m, nth):
        rel = rels[nth]
        sl, k = cl * per + m, cl * two + 2 * m + role
        back = (n_ctx - rel) % n_ctx
        norm = l_st[nth][:, :1]
        live = norm > 0.0
        safe = jnp.where(live, norm, 1.0)
        o = (acc[nth] * (1.0 / safe)).astype(jnp.bfloat16)
        norm = l_st[nth]
        lse = jnp.where(norm > 0.0, m_st[nth] + jnp.log2(jnp.where(norm > 0.0, norm, 1.0)), NEG)
        for rr in (0, 1):
            piece = o[rr * rows:(rr + 1) * rows]
            e = lse[rr * rows:(rr + 1) * rows].T[:8]
            if rel == 0 and rr == 0:
                o_in[k, 0] = piece
                e_in[k, 0] = e
                continue
            o_out[sl, rel * 2 + rr] = piece
            e_out[sl, rel * 2 + rr] = e
        for rr in (0, 1):
            if rel == 0 and rr == 0:
                continue
            dev = (role_at(rr), ctx_at(rel), req)
            n = ocount[0]
            send(e_out.at[sl, rel * 2 + rr], e_in.at[k, back], o_ss.at[n, 1], o_rs.at[k, back, 1], dev)
            send(o_out.at[sl, rel * 2 + rr], o_in.at[k, back], o_ss.at[n, 0], o_rs.at[k, back, 0], dev)
            ocount[0] += 1

    def parts_of(cl, m, first, last):
        def body(p, carry):
            await_part(cl, m, p)
            for nth in range(n_ctx):
                part(cl, m, p, nth)
            return carry
        lax.fori_loop(first, last, body, 0)

    def last_part(cl, m, p):
        p = jnp.int32(p)
        await_part(cl, m, p)
        for nth in range(n_ctx):
            part(cl, m, p, nth)
            close_block(cl, m, nth)

    out_rows = lax.broadcasted_iota(jnp.int32, (two * block, 128), 0)
    which = lax.div(lax.rem(out_rows, block), steps)
    guarded = []

    def spread(row):
        return jnp.broadcast_to(row[:1], (128, rows)).T

    def merge(cl):
        for rr in (0, 1):
            for m in range(per):
                k = cl * two + 2 * m + role_at(rr)
                for rel in range(n_ctx):
                    if rr or rel:
                        arrived(o_in.at[k, rel], o_rs.at[k, rel, 0])
                        arrived(e_in.at[k, rel], o_rs.at[k, rel, 1])
                es = [e_in[k, rel] for rel in range(n_ctx)]
                top = functools.reduce(jnp.maximum, es)
                shares = [jnp.exp2(e - top) for e in es]
                norm = sum(shares)
                f_out[k] = top + jnp.log2(norm)
                value = 0.0
                for rel in range(n_ctx):
                    w = jnp.concatenate([spread(shares[rel] / norm)] * (latent // 128), axis=1)
                    value = value + o_in[k, rel].astype(jnp.float32) * w
                merged[k] = value.astype(jnp.bfloat16)

        def up(hb, carry):
            r0 = pl.multiple_of(hb * block, block)
            lhs = jnp.concatenate([merged[cl * two + k, pl.ds(r0, block), :] for k in range(two)], axis=0)
            res = jnp.zeros((two * block, 128), jnp.float32)
            for j in range(BLOCK_HEADS):
                one = jnp.dot(lhs, vu_v[head_at(hb, j)], preferred_element_type=jnp.float32)
                res = jnp.where(which == j, one, res)
            res = res.astype(jnp.bfloat16)
            for k in range(two):
                att_out[cl * two + k, pl.ds(r0, block), :] = res[k * block:(k + 1) * block]
            return carry

        lax.fori_loop(0, heads // BLOCK_HEADS, up, 0)
        for k in range(two):
            e = cl * two + k
            owner = owner_of(cl, jnp.int32(k), req)
            if cl == 0:
                at, dst, fdst, sems = hi, att_a, f_a, ta_rs
            elif cl == 1:
                at, dst, fdst, sems = lax.div(req, 2), att_b, f_b, tb_rs
            else:
                at, dst, fdst, sems = lax.rem(req, 2) + 2 * hi, att_b, f_b, tb_rs
            copies = [
                pltpu.make_async_remote_copy(
                    src_ref=src.at[e], dst_ref=d.at[at], send_sem=t_ss.at[e, j], recv_sem=sems.at[at, j],
                    device_id=(role, ctx, owner), device_id_type=MESH)
                for j, (src, d) in enumerate(((att_out, dst), (f_out, fdst)))
            ]

            @pl.when(owner != req)
            def _():
                for copy in copies:
                    copy.start()

            @pl.when(owner == req)
            def _():
                dst[at] = att_out[e]
                fdst[at] = f_out[e]
            guarded.append((owner, copies))

    own_b = jnp.where(bit2 == 0, lax.div(req, 2), lax.rem(req, 2) + 2 * hi)

    def combine(slot):
        count, src, fsrc, sems, mine = ((high, att_a, f_a, ta_rs, hi), (4 * per, att_b, f_b, tb_rs, own_b))[slot]
        for j in range(count):
            @pl.when(mine != j)
            def _():
                arrived(src.at[j], sems.at[j, 0])
                arrived(fsrc.at[j], sems.at[j, 1])
        es = [fsrc[j] for j in range(count)]
        top = functools.reduce(jnp.maximum, es)
        shares = [jnp.exp2(e - top) for e in es]
        norm = sum(shares)
        value = 0.0
        for j in range(count):
            value = value + src[j].astype(jnp.float32) * spread(shares[j] / norm)
        fin[slot] = value
        for h in range(heads):
            r = first_row(h)
            out_ref[slot, :, h * 128:(h + 1) * 128] = fin[slot, r:r + steps, :].astype(jnp.bfloat16)

    for cl in (1, 2):
        for m in range(per):
            open_slot(cl, m)
            parts_of(cl, m, 0, 1)
            last_part(cl, m, 1)
    for m in range(per):
        open_slot(0, m)
        parts_of(0, m, 0, 3)
        if m == per - 1:
            loads[2].wait()
            merge(1)
            merge(2)
        last_part(0, m, 3)
    combine(1)
    merge(0)
    combine(0)

    for copy in started:
        copy.wait_send()
    for owner, copies in guarded:
        @pl.when(owner != req)
        def _():
            for copy in copies:
                copy.wait_send()


def shards(cache, lengths, request_decode_slot, q_nope, q_rope, new_latent, w_key, value_up_weight):
    total = request_decode_slot.shape[0]
    n_req, n_ctx = lax.axis_size("req"), lax.axis_size("ctx")
    heads, nope, latent = w_key.shape
    vdim = value_up_weight.shape[2]
    own, steps = q_nope.shape[:2]
    rope = q_rope.shape[2] // heads
    span, half = cache.shape[1:]
    rows = heads * steps
    per, two, high = n_req // 8, n_req // 4, n_req // 4
    groups = 2 * n_ctx
    scale2 = (nope + rope) ** (-0.5) * math.log2(math.e)

    turned = jnp.swapaxes(cache, 1, 2)
    bf, f32 = jnp.bfloat16, jnp.float32
    chunks = total - 3 * per
    vm, dma = pltpu.VMEM, pltpu.SemaphoreType.DMA
    smem = pl.BlockSpec(memory_space=pltpu.SMEM)
    here = pl.BlockSpec(memory_space=pltpu.VMEM)
    away = pl.BlockSpec(memory_space=pl.ANY)
    return pl.pallas_call(
        functools.partial(kernel, (n_req, n_ctx, scale2)),
        out_shape=jax.ShapeDtypeStruct((own, steps, heads * vdim), bf),
        in_specs=[smem, smem, away, here, here, here, away, away],
        out_specs=here,
        scratch_shapes=[
            vm((total, half, span), bf),
            vm((chunks, half, span), bf),
            vm((per, 4, 2 * half, span), bf),
            vm((2 * per, 2, 2 * half, span), bf),
            vm(w_key.shape, bf),
            vm(value_up_weight.shape, bf),
            vm((own, rows, nope), f32),
            vm((own, rows // 2, 2 * rope), f32),
            vm((own, rows, nope), bf),
            vm((own, rows // 2, 2 * rope), bf),
            vm((own, 128, latent + 2 * rope), f32),
            vm((3 * two, rows, nope), bf),
            vm((3 * two, rows // 2, 2 * rope), bf),
            vm((3 * two, rows, latent), bf),
            vm((3 * per, groups, rows, latent), bf),
            vm((3 * per, groups, rows // 2, 2 * rope), bf),
            vm((n_ctx, 2 * rows, 128), f32),
            vm((n_ctx, 2 * rows, 128), f32),
            vm((n_ctx, 2 * rows, latent), f32),
            vm((3 * per, groups, rows, latent), bf),
            vm((3 * per, groups, 8, rows), f32),
            vm((3 * two, n_ctx, rows, latent), bf),
            vm((3 * two, n_ctx, 8, rows), f32),
            vm((3 * two, rows, latent), bf),
            vm((3 * two, rows, vdim), bf),
            vm((3 * two, 8, rows), f32),
            vm((high, rows, vdim), bf),
            vm((high, 8, rows), f32),
            vm((4 * per, rows, vdim), bf),
            vm((4 * per, 8, rows), f32),
            vm((own, rows, vdim), f32),
            dma((3,)),
            dma((3 * high, 2)),
            dma((3 * two, 2)),
            dma((chunks,)),
            dma((per, 4, 2)),
            dma((2 * per, 2, 2)),
            dma((3 * per * (groups - 1), 2)),
            dma((3 * per, groups, 2)),
            dma((3 * per * (groups - 1), 2)),
            dma((3 * two, n_ctx, 2)),
            dma((3 * two, 2)),
            dma((high, 2)),
            dma((4 * per, 2)),
        ],
        compiler_params=pltpu.CompilerParams(
            collective_id=0, has_side_effects=True, vmem_limit_bytes=62 * 1024 * 1024
        ),
    )(request_decode_slot, lengths, turned, q_nope, q_rope, new_latent, w_key, value_up_weight)


def solution(mesh):
    placed = (
        P(None, ("ctx", "req"), "role"),
        P(),
        P(),
        P("req", None, ("role", "ctx")),
        P("req", None, ("role", "ctx")),
        P("req", None, None),
        P(("role", "ctx"), None, None),
        P(("role", "ctx"), None, None),
    )
    return jax.shard_map(
        shards,
        mesh=mesh,
        in_specs=placed,
        out_specs=P("req", None, ("role", "ctx")),
        check_vma=False,
    )
```

```python
import functools
import math

import jax
import jax.numpy as jnp
from jax import lax
from jax.experimental import pallas as pl
from jax.experimental.pallas import tpu as pltpu
from jax.sharding import PartitionSpec as P

NEG = -1e30
LOW = -1e29
MESH = pl.DeviceIdType.MESH
BLOCK_HEADS = 4
UNROLL = 4


def xor_bit(value, bit, flip):
    b = lax.rem(lax.div(value, bit), 2)
    return value + flip * bit * (1 - 2 * b)


def owner_of(cl, k, chip):
    if cl == 0:
        return lax.rem(chip, 4) + 4 * k
    if cl == 1:
        return lax.rem(chip, 2) + 2 * lax.rem(k, 2) + 8 * lax.div(k, 2)
    return lax.rem(k, 2) + 2 * lax.rem(lax.div(chip, 2), 2) + 4 + 8 * lax.div(k, 2)


def neighbour(cl, p, chip):
    if cl == 0:
        return xor_bit(xor_bit(chip, 1, p % 2), 2, p // 2)
    return xor_bit(chip, cl, p)


def kernel(dims, slot_ref, len_ref, cache_ref, qn_any, qr_any, new_any, wk_ref, vu_ref, out_ref,
           qn_ref, qr_ref, new_ref, cache_v, ksend, k_a, k_b, wk_v, vu_v, qn_f, qr_f, qn_s, qr_s, new_f, rawn, rawr, qa, q_in, r_in,
           m_st, l_st, acc, o_out, e_out, o_in, e_in, merged, att_out, f_out, att_a, f_a, att_b, f_b, fin,
           load_sem, cache_sem, raw_ss, raw_rs, k_ss, ka_rs, kb_rs, q_ss, q_rs, o_ss, o_rs, t_ss, ta_rs, tb_rs):
    n_req, n_ctx, scale2 = dims
    role, ctx, req = lax.axis_index("role"), lax.axis_index("ctx"), lax.axis_index("req")
    per = n_req // 8
    two = 2 * per
    high = n_req // 4
    total, half, span = cache_ref.shape
    heads, nope, latent = wk_ref.shape
    own, steps = qn_any.shape[:2]
    rows = heads * steps
    pairs = heads // 2
    low, hi = lax.rem(req, 4), lax.div(req, 4)
    bit2 = lax.rem(hi, 2)
    other = 1 - role

    def role_at(rr):
        return role if rr == 0 else other

    def ctx_at(t):
        return lax.rem(ctx + t, n_ctx)

    caches = [pltpu.make_async_copy(cache_ref.at[r], cache_v.at[r], cache_sem.at[r]) for r in range(total)]
    loads = [None,
             pltpu.make_async_copy(wk_ref, wk_v, load_sem.at[1]),
             pltpu.make_async_copy(vu_ref, vu_v, load_sem.at[2]),
             pltpu.make_async_copy(qn_any, qn_ref, load_sem.at[3]),
             pltpu.make_async_copy(qr_any, qr_ref, load_sem.at[4]),
             pltpu.make_async_copy(new_any, new_ref, load_sem.at[5])]
    for one in (3, 4, 5):
        loads[one].start()
    for copy in caches:
        copy.start()

    partners = []
    for d in (1, 2, 3):
        for rr in (0, 1):
            partners.append((role_at(rr), ctx, neighbour(0, d, req)))
    for t in range(n_ctx):
        for rr in (0, 1):
            if t or rr:
                partners.append((role_at(rr), ctx_at(t), req))
    for v in range(1, high):
        far = 4 * lax.rem(hi + v, high)
        for d in (0, 1, 2):
            partners.append((role, ctx, neighbour(0, d, low) + far))
    barrier = pltpu.get_barrier_semaphore()
    for dev in partners:
        pl.semaphore_signal(barrier, inc=1, device_id=dev, device_id_type=MESH)

    started = []

    def send(src, dst, ss, rs, dev):
        copy = pltpu.make_async_remote_copy(src_ref=src, dst_ref=dst, send_sem=ss, recv_sem=rs, device_id=dev,
                                            device_id_type=MESH)
        copy.start()
        started.append(copy)

    def arrived(ref, sem):
        pltpu.make_async_copy(ref, ref, sem).wait()

    def first_row(h):
        return ((h % 2) * pairs + h // 2) * steps

    for one in (3, 4, 5):
        loads[one].wait()
    for slot in range(own):
        for h in range(heads):
            r = first_row(h)
            qn_f[slot, r:r + steps, :] = qn_ref[slot, :, h * nope:(h + 1) * nope].astype(jnp.float32)
        for h in range(pairs):
            qr_f[slot, h * steps:(h + 1) * steps, :] = qr_ref[slot, :, h * 128:(h + 1) * 128].astype(jnp.float32)
        qn_s[slot] = qn_f[slot].astype(jnp.bfloat16)
        qr_s[slot] = qr_f[slot].astype(jnp.bfloat16)
    new_f[...] = jnp.zeros_like(new_f)
    for slot in range(own):
        fresh_rows = new_ref[slot].astype(jnp.float32)
        new_f[slot, :steps, :latent] = fresh_rows[:, :latent]
        new_f[slot, :steps, latent:] = jnp.concatenate([fresh_rows[:, latent:]] * 2, axis=1)

    def request_of(slot):
        def body(j, acc_):
            return jnp.where(slot_ref[j] == slot, j, acc_)
        if total <= 16:
            r = jnp.int32(0)
            for j in range(total):
                r = body(j, r)
            return r
        return lax.fori_loop(0, total, body, jnp.int32(0))

    def k_ref(cl, m, p):
        return k_a.at[m, p] if cl == 0 else k_b.at[(cl - 1) * per + m, p]

    def k_sem(cl, m, p, h):
        return ka_rs.at[m, p, h] if cl == 0 else kb_rs.at[(cl - 1) * per + m, p, h]

    mine_rows = pl.ds(pl.multiple_of(role * half, 16), half)
    order = [(1, 1), (2, 1), (0, 1), (0, 2), (0, 3), (1, 0), (2, 0), (0, 0)]
    todo, lengths = [], {}
    for cl, p in order:
        for to in ((0, 1) if p else (role, other)):
            for m in range(per):
                chip = neighbour(cl, p, req)
                slot = 2 * owner_of(cl, 2 * m + to, chip) + (1 if cl else 0)
                todo.append((cl, p, to, m, chip, request_of(slot)))
    for copy in caches:
        copy.wait()
    loads[1].start()
    loads[2].start()
    pending, delayed = [], []
    chunk = 0
    for cl, p, to, m, chip, request in todo:
        dst = k_ref(cl, m, p)
        if to is role:
            dst[mine_rows, :] = cache_v[request]
            lengths[cl, m] = len_ref[request]
            continue
        ksend[chunk] = cache_v[request]
        first = m == 0 and cl > 0 and p > 0
        split = first and p > 0 and to == 1
        cut = half // 32 * 16 if split else half
        for begin, end, early in ((0, cut, first), (cut, half, False)):
            if begin < end:
                rows_to = pl.ds(pl.multiple_of(role * half + begin, 16), end - begin)
                (pending if early else delayed).append(
                    (ksend.at[chunk, pl.ds(begin, end - begin)], dst.at[rows_to, :],
                     k_ss.at[chunk, 0 if early else 1], k_sem(cl, m, p, role), (to, ctx, chip)))
        chunk += 1

    kk = jnp.where(bit2 == 0, lax.rem(lax.div(req, 2), 2), lax.rem(req, 2)) + 2 * lax.div(req, 8)
    mine_a, mine_b = (0, hi), (1 + bit2, kk)
    for slot, (cl, k) in ((0, mine_a), (1, mine_b)):
        rawn[cl * two + k] = qn_s[slot]
        rawr[cl * two + k] = qr_s[slot]

    pl.semaphore_wait(barrier, len(partners))

    rcount = [0]

    def share_raw(n_src, r_src, spot, dev):
        n = rcount[0]
        send(n_src, rawn.at[spot], raw_ss.at[n, 0], raw_rs.at[spot, 0], dev)
        send(r_src, rawr.at[spot], raw_ss.at[n, 1], raw_rs.at[spot, 1], dev)
        rcount[0] += 1

    def flipped(chip, bit):
        return jnp.where(bit == 0, xor_bit(chip, 2, 1), xor_bit(chip, 1, 1))

    spot_a, spot_b = hi, (1 + bit2) * two + kk
    for v in range(1, high):
        chip = low + 4 * lax.rem(hi + v, high)
        share_raw(qn_s.at[1], qr_s.at[1], spot_b, (role, ctx, chip))
        share_raw(qn_s.at[0], qr_s.at[0], spot_a, (role, ctx, chip))
    share_raw(qn_s.at[1], qr_s.at[1], spot_b, (role, ctx, flipped(req, bit2)))
    for one in pending:
        send(*one)

    block = BLOCK_HEADS * steps
    half_blocks = pairs // BLOCK_HEADS

    def head_at(hb, j):
        return 2 * (BLOCK_HEADS * lax.rem(hb, half_blocks) + j) + lax.div(hb, half_blocks)

    def absorb(batch):
        shape = (len(batch) * block, BLOCK_HEADS * nope)
        of_row = lax.div(lax.rem(lax.broadcasted_iota(jnp.int32, shape, 0), block), steps)
        of_col = lax.div(lax.broadcasted_iota(jnp.int32, shape, 1), nope)
        diagonal = (of_row == of_col).astype(jnp.float32).astype(jnp.bfloat16)

        def body(hb, carry):
            r0 = pl.multiple_of(hb * block, block)
            lhs = jnp.concatenate([rawn[cl * two + k, pl.ds(r0, block), :] for cl, k in batch], axis=0)
            lhs = jnp.concatenate([lhs] * BLOCK_HEADS, axis=1) * diagonal
            w = jnp.concatenate([wk_v[head_at(hb, j)] for j in range(BLOCK_HEADS)], axis=0)
            res = jnp.dot(lhs, w, preferred_element_type=jnp.float32).astype(jnp.bfloat16)
            for n, (cl, k) in enumerate(batch):
                qa[cl * two + k, pl.ds(r0, block), :] = res[n * block:(n + 1) * block]
            return carry

        lax.fori_loop(0, heads // BLOCK_HEADS, body, 0, unroll=UNROLL)

    guarded = []
    qcount = [0]

    def share_queries(batch):
        for cl, k in batch:
            e, to = cl * two + k, lax.rem(k, 2)
            sl, rr = cl * per + lax.div(k, 2), lax.rem(to + role, 2)
            for t in list(range(1, n_ctx)) + [0]:
                at = ((n_ctx - t) % n_ctx) * 2 + rr
                n = qcount[0]
                copies = [
                    pltpu.make_async_remote_copy(
                        src_ref=src.at[e], dst_ref=dst.at[sl, at], send_sem=q_ss.at[n, j], recv_sem=q_rs.at[sl, at, j],
                        device_id=(to, ctx_at(t), req), device_id_type=MESH)
                    for j, (src, dst) in ((1, (rawr, r_in)), (0, (qa, q_in)))
                ]
                if t:
                    for copy in copies:
                        copy.start()
                    started.extend(copies)
                else:
                    away = to != role

                    @pl.when(away)
                    def _():
                        for copy in copies:
                            copy.start()
                    guarded.append((away, copies))
                qcount[0] += 1

    def raw_arrived(cl, k):
        arrived(rawn.at[cl * two + k], raw_rs.at[cl * two + k, 0])
        arrived(rawr.at[cl * two + k], raw_rs.at[cl * two + k, 1])

    def class_b(owner):
        bit = lax.rem(lax.div(owner, 4), 2)
        place = jnp.where(bit == 0, lax.rem(lax.div(owner, 2), 2), lax.rem(owner, 2))
        return bit, (1 + bit, place + 2 * lax.div(owner, 8))

    loads[1].wait()
    absorb([mine_b, mine_a])
    share_queries([mine_b, mine_a])
    near, far = [class_b(flipped(req, bit2))[1]], []
    for v in range(1, high):
        owner = low + 4 * lax.rem(hi + v, high)
        bit, entry = class_b(owner)
        raw_arrived(*entry)
        spot = entry[0] * two + entry[1]
        share_raw(rawn.at[spot], rawr.at[spot], spot, (role, ctx, flipped(req, bit)))
        near.append(entry)
        far.append(class_b(flipped(owner, bit))[1])
    for one in delayed:
        send(*one)
    for v in range(1, high):
        entry = (0, lax.rem(hi + v, high))
        raw_arrived(*entry)
        near.append(entry)
    raw_arrived(*near[0])
    absorb(near)
    share_queries(near)
    for entry in far:
        raw_arrived(*entry)
    absorb(far)
    share_queries(far)

    nt = (((1,), (1,)), ((), ()))
    rels = list(range(1, n_ctx)) + [0]
    lane = lax.broadcasted_iota(jnp.int32, (rows // 2, 128), 1)
    even = (lane < 64).astype(jnp.float32).astype(jnp.bfloat16)
    odd = (lane >= 64).astype(jnp.float32).astype(jnp.bfloat16)

    def queries(cl, m, rel):
        sl, k = cl * per + m, cl * two + 2 * m + role
        if rel == 0:
            q_own, r_own = qa[k], rawr[k]
        else:
            q_own, r_own = q_in[sl, rel * 2], r_in[sl, rel * 2]
        r_far = r_in[sl, rel * 2 + 1]
        q = jnp.concatenate([q_own, q_in[sl, rel * 2 + 1]], axis=0)
        qr = jnp.concatenate([r_own * even, r_own * odd, r_far * even, r_far * odd], axis=0)
        return q, qr

    def open_slot(cl, m):
        sl = cl * per + m
        fresh_on = jnp.logical_and(owner_of(cl, 2 * m + role, req) == req, ctx == 0)
        new = new_f[1 if cl else 0].astype(jnp.bfloat16)
        for nth, rel in enumerate(rels):
            for rr in (0, 1):
                if rel or rr:
                    arrived(q_in.at[sl, rel * 2 + rr], q_rs.at[sl, rel * 2 + rr, 0])
                    arrived(r_in.at[sl, rel * 2 + rr], q_rs.at[sl, rel * 2 + rr, 1])
            q, qr = queries(cl, m, rel)
            fresh = (lax.dot_general(q, new[:, :latent], nt, preferred_element_type=jnp.float32)
                     + lax.dot_general(qr, new[:, latent:], nt, preferred_element_type=jnp.float32)) * scale2
            token = lax.broadcasted_iota(jnp.int32, fresh.shape, 1)
            step = lax.rem(lax.broadcasted_iota(jnp.int32, fresh.shape, 0), steps)
            fresh = jnp.where(token <= jnp.where(fresh_on, step, -1), fresh, NEG)
            top = jnp.maximum(jnp.max(fresh, axis=1, keepdims=True), LOW)
            weights = jnp.exp2(fresh - top)
            m_st[nth] = jnp.broadcast_to(top, (2 * rows, 128))
            l_st[nth] = jnp.broadcast_to(jnp.sum(weights, axis=1, keepdims=True), (2 * rows, 128))
            acc[nth] = jnp.dot(weights.astype(jnp.bfloat16), new[:, :latent], preferred_element_type=jnp.float32)

    def await_part(cl, m, p):
        sample = k_ref(cl, m, 0).at[pl.ds(0, half), :]

        @pl.when(p > 0)
        def _():
            arrived(sample, k_sem(cl, m, p, role))
        arrived(sample, k_sem(cl, m, p, other))

    def part(cl, m, p, nth):
        q, qr = queries(cl, m, rels[nth])
        keys = k_ref(cl, m, p)
        rotary = keys[latent:, :]
        s = jnp.dot(q, keys[:latent, :], preferred_element_type=jnp.float32)
        s += jnp.dot(qr, jnp.concatenate([rotary, rotary], axis=0), preferred_element_type=jnp.float32)
        if cl == 0:
            chip = xor_bit(xor_bit(req, 1, lax.rem(p, 2)), 2, lax.div(p, 2))
        else:
            chip = xor_bit(req, cl, p)
        position = (ctx * n_req + chip) * span + lax.broadcasted_iota(jnp.int32, (1, span), 1)
        s = jnp.where(position < lengths[cl, m], s * scale2, NEG)
        before = m_st[nth][:, :1]
        top = jnp.maximum(before, jnp.max(s, axis=1, keepdims=True))
        keep = jnp.exp2(before - top)
        w = jnp.exp2(s - top)
        m_st[nth] = jnp.broadcast_to(top, (2 * rows, 128))
        l_st[nth] = l_st[nth] * keep + jnp.sum(w, axis=1, keepdims=True)
        acc[nth] = acc[nth] * keep + lax.dot_general(w.astype(jnp.bfloat16), keys[:latent, :], nt,
                                                     preferred_element_type=jnp.float32)

    ocount = [0]

    def close_block(cl, m, nth):
        rel = rels[nth]
        sl, k = cl * per + m, cl * two + 2 * m + role
        back = (n_ctx - rel) % n_ctx
        norm = l_st[nth][:, :1]
        live = norm > 0.0
        safe = jnp.where(live, norm, 1.0)
        o = (acc[nth] * (1.0 / safe)).astype(jnp.bfloat16)
        norm = l_st[nth]
        lse = jnp.where(norm > 0.0, m_st[nth] + jnp.log2(jnp.where(norm > 0.0, norm, 1.0)), NEG)
        for rr in (0, 1):
            piece = o[rr * rows:(rr + 1) * rows]
            e = lse[rr * rows:(rr + 1) * rows].T[:8]
            if rel == 0 and rr == 0:
                o_in[k, 0] = piece
                e_in[k, 0] = e
                continue
            o_out[sl, rel * 2 + rr] = piece
            e_out[sl, rel * 2 + rr] = e
        for rr in (0, 1):
            if rel == 0 and rr == 0:
                continue
            dev = (role_at(rr), ctx_at(rel), req)
            n = ocount[0]
            send(e_out.at[sl, rel * 2 + rr], e_in.at[k, back], o_ss.at[n, 1], o_rs.at[k, back, 1], dev)
            send(o_out.at[sl, rel * 2 + rr], o_in.at[k, back], o_ss.at[n, 0], o_rs.at[k, back, 0], dev)
            ocount[0] += 1

    def parts_of(cl, m, first, last):
        def body(p, carry):
            await_part(cl, m, p)
            for nth in range(n_ctx):
                part(cl, m, p, nth)
            return carry
        lax.fori_loop(first, last, body, 0)

    def last_part(cl, m, p):
        p = jnp.int32(p)
        await_part(cl, m, p)
        for nth in range(n_ctx):
            part(cl, m, p, nth)
            close_block(cl, m, nth)

    out_rows = lax.broadcasted_iota(jnp.int32, (two * block, 128), 0)
    which = lax.div(lax.rem(out_rows, block), steps)
    def spread(row):
        return jnp.broadcast_to(row[:1], (128, rows)).T

    def merge(cl):
        for rr in (0, 1):
            for m in range(per):
                k = cl * two + 2 * m + role_at(rr)
                for rel in range(n_ctx):
                    if rr or rel:
                        arrived(o_in.at[k, rel], o_rs.at[k, rel, 0])
                        arrived(e_in.at[k, rel], o_rs.at[k, rel, 1])
                es = [e_in[k, rel] for rel in range(n_ctx)]
                top = functools.reduce(jnp.maximum, es)
                shares = [jnp.exp2(e - top) for e in es]
                norm = sum(shares)
                f_out[k] = top + jnp.log2(norm)
                value = 0.0
                for rel in range(n_ctx):
                    w = jnp.concatenate([spread(shares[rel] / norm)] * (latent // 128), axis=1)
                    value = value + o_in[k, rel].astype(jnp.float32) * w
                merged[k] = value.astype(jnp.bfloat16)

        def up(hb, carry):
            r0 = pl.multiple_of(hb * block, block)
            lhs = jnp.concatenate([merged[cl * two + k, pl.ds(r0, block), :] for k in range(two)], axis=0)
            res = jnp.zeros((two * block, 128), jnp.float32)
            for j in range(BLOCK_HEADS):
                one = jnp.dot(lhs, vu_v[head_at(hb, j)], preferred_element_type=jnp.float32)
                res = jnp.where(which == j, one, res)
            res = res.astype(jnp.bfloat16)
            for k in range(two):
                att_out[cl * two + k, pl.ds(r0, block), :] = res[k * block:(k + 1) * block]
            return carry

        lax.fori_loop(0, heads // BLOCK_HEADS, up, 0, unroll=UNROLL)
        for k in range(two):
            e = cl * two + k
            owner = owner_of(cl, jnp.int32(k), req)
            if cl == 0:
                at, dst, fdst, sems = hi, att_a, f_a, ta_rs
            elif cl == 1:
                at, dst, fdst, sems = lax.div(req, 2), att_b, f_b, tb_rs
            else:
                at, dst, fdst, sems = lax.rem(req, 2) + 2 * hi, att_b, f_b, tb_rs
            copies = [
                pltpu.make_async_remote_copy(
                    src_ref=src.at[e], dst_ref=d.at[at], send_sem=t_ss.at[e, j], recv_sem=sems.at[at, j],
                    device_id=(role, ctx, owner), device_id_type=MESH)
                for j, (src, d) in enumerate(((att_out, dst), (f_out, fdst)))
            ]

            @pl.when(owner != req)
            def _():
                for copy in copies:
                    copy.start()

            @pl.when(owner == req)
            def _():
                dst[at] = att_out[e]
                fdst[at] = f_out[e]
            guarded.append((owner != req, copies))

    own_b = jnp.where(bit2 == 0, lax.div(req, 2), lax.rem(req, 2) + 2 * hi)

    def combine(slot):
        count, src, fsrc, sems, mine = ((high, att_a, f_a, ta_rs, hi), (4 * per, att_b, f_b, tb_rs, own_b))[slot]
        for j in range(count):
            @pl.when(mine != j)
            def _():
                arrived(src.at[j], sems.at[j, 0])
                arrived(fsrc.at[j], sems.at[j, 1])
        es = [fsrc[j] for j in range(count)]
        top = functools.reduce(jnp.maximum, es)
        shares = [jnp.exp2(e - top) for e in es]
        norm = sum(shares)
        value = 0.0
        for j in range(count):
            value = value + src[j].astype(jnp.float32) * spread(shares[j] / norm)
        fin[slot] = value
        for h in range(heads):
            r = first_row(h)
            out_ref[slot, :, h * 128:(h + 1) * 128] = fin[slot, r:r + steps, :].astype(jnp.bfloat16)

    for cl in (1, 2):
        for m in range(per):
            open_slot(cl, m)
            parts_of(cl, m, 0, 1)
            last_part(cl, m, 1)
    for m in range(per):
        open_slot(0, m)
        parts_of(0, m, 0, 3)
        if m == per - 1:
            loads[2].wait()
            merge(1)
            merge(2)
        last_part(0, m, 3)
    combine(1)
    merge(0)
    combine(0)

    for copy in started:
        copy.wait_send()
    for sent, copies in guarded:
        @pl.when(sent)
        def _():
            for copy in copies:
                copy.wait_send()


def shards(cache, lengths, request_decode_slot, q_nope, q_rope, new_latent, w_key, value_up_weight):
    total = request_decode_slot.shape[0]
    n_req, n_ctx = lax.axis_size("req"), lax.axis_size("ctx")
    heads, nope, latent = w_key.shape
    vdim = value_up_weight.shape[2]
    own, steps = q_nope.shape[:2]
    rope = q_rope.shape[2] // heads
    span, half = cache.shape[1:]
    rows = heads * steps
    per, two, high = n_req // 8, n_req // 4, n_req // 4
    groups = 2 * n_ctx
    scale2 = (nope + rope) ** (-0.5) * math.log2(math.e)

    turned = jnp.swapaxes(cache, 1, 2)
    bf, f32 = jnp.bfloat16, jnp.float32
    chunks = total - 3 * per
    vm, dma = pltpu.VMEM, pltpu.SemaphoreType.DMA
    smem = pl.BlockSpec(memory_space=pltpu.SMEM)
    away = pl.BlockSpec(memory_space=pl.ANY)
    out = pl.pallas_call(
        functools.partial(kernel, (n_req, n_ctx, scale2)),
        out_shape=pltpu.VMEM((own, steps, heads * vdim), bf),
        in_specs=[smem, smem, away, away, away, away, away, away],
        out_specs=pl.BlockSpec(memory_space=pltpu.VMEM),
        scratch_shapes=[
            vm(q_nope.shape, bf),
            vm(q_rope.shape, bf),
            vm(new_latent.shape, bf),
            vm((total, half, span), bf),
            vm((chunks, half, span), bf),
            vm((per, 4, 2 * half, span), bf),
            vm((2 * per, 2, 2 * half, span), bf),
            vm(w_key.shape, bf),
            vm(value_up_weight.shape, bf),
            vm((own, rows, nope), f32),
            vm((own, rows // 2, 2 * rope), f32),
            vm((own, rows, nope), bf),
            vm((own, rows // 2, 2 * rope), bf),
            vm((own, 128, latent + 2 * rope), f32),
            vm((3 * two, rows, nope), bf),
            vm((3 * two, rows // 2, 2 * rope), bf),
            vm((3 * two, rows, latent), bf),
            vm((3 * per, groups, rows, latent), bf),
            vm((3 * per, groups, rows // 2, 2 * rope), bf),
            vm((n_ctx, 2 * rows, 128), f32),
            vm((n_ctx, 2 * rows, 128), f32),
            vm((n_ctx, 2 * rows, latent), f32),
            vm((3 * per, groups, rows, latent), bf),
            vm((3 * per, groups, 8, rows), f32),
            vm((3 * two, n_ctx, rows, latent), bf),
            vm((3 * two, n_ctx, 8, rows), f32),
            vm((3 * two, rows, latent), bf),
            vm((3 * two, rows, vdim), bf),
            vm((3 * two, 8, rows), f32),
            vm((high, rows, vdim), bf),
            vm((high, 8, rows), f32),
            vm((4 * per, rows, vdim), bf),
            vm((4 * per, 8, rows), f32),
            vm((own, rows, vdim), f32),
            dma((6 + own,)),
            dma((total,)),
            dma((3 * high, 2)),
            dma((3 * two, 2)),
            dma((chunks, 2)),
            dma((per, 4, 2)),
            dma((2 * per, 2, 2)),
            dma((3 * two * n_ctx, 2)),
            dma((3 * per, groups, 2)),
            dma((3 * per * (groups - 1), 2)),
            dma((3 * two, n_ctx, 2)),
            dma((3 * two, 2)),
            dma((high, 2)),
            dma((4 * per, 2)),
        ],
        compiler_params=pltpu.CompilerParams(
            collective_id=0, has_side_effects=True, vmem_limit_bytes=62 * 1024 * 1024
        ),
    )(request_decode_slot, lengths, turned, q_nope, q_rope, new_latent, w_key, value_up_weight)
    return out


def solution(mesh):
    placed = (
        P(None, ("ctx", "req"), "role"),
        P(),
        P(),
        P("req", None, ("role", "ctx")),
        P("req", None, ("role", "ctx")),
        P("req", None, None),
        P(("role", "ctx"), None, None),
        P(("role", "ctx"), None, None),
    )
    return jax.shard_map(
        shards,
        mesh=mesh,
        in_specs=placed,
        out_specs=P("req", None, ("role", "ctx")),
        check_vma=False,
    )
```

```python
import functools
import math

import jax
import jax.numpy as jnp
from jax import lax
from jax.experimental import pallas as pl
from jax.experimental.pallas import tpu as pltpu
from jax.sharding import PartitionSpec as P

NEG = -1e30
LOW = -1e29
MESH = pl.DeviceIdType.MESH
BLOCK_HEADS = 4
UNROLL = 8


def xor_bit(value, bit, flip):
    b = lax.rem(lax.div(value, bit), 2)
    return value + flip * bit * (1 - 2 * b)


def owner_of(cl, k, chip):
    if cl == 0:
        return lax.rem(chip, 4) + 4 * k
    if cl == 1:
        return lax.rem(chip, 2) + 2 * lax.rem(k, 2) + 8 * lax.div(k, 2)
    return lax.rem(k, 2) + 2 * lax.rem(lax.div(chip, 2), 2) + 4 + 8 * lax.div(k, 2)


def neighbour(cl, p, chip):
    if cl == 0:
        return xor_bit(xor_bit(chip, 1, p % 2), 2, p // 2)
    return xor_bit(chip, cl, p)


def kernel(dims, slot_ref, len_ref, cache_ref, qn_any, qr_any, new_any, wk_ref, vu_ref, out_ref,
           qn_ref, qr_ref, new_ref, cache_v, ksend, k_a, k_b, wk_v, vu_v, qn_f, qr_f, qn_s, qr_s, new_f, rawn, rawr, qa, q_in, r_in,
           m_st, l_st, acc, o_out, e_out, o_in, e_in, merged, att_out, f_out, att_a, f_a, att_b, f_b, fin,
           load_sem, cache_sem, raw_ss, raw_rs, k_ss, ka_rs, kb_rs, q_ss, q_rs, o_ss, o_rs, t_ss, ta_rs, tb_rs):
    n_req, n_ctx, scale2 = dims
    role, ctx, req = lax.axis_index("role"), lax.axis_index("ctx"), lax.axis_index("req")
    per = n_req // 8
    two = 2 * per
    high = n_req // 4
    total, half, span = cache_ref.shape
    heads, nope, latent = wk_ref.shape
    own, steps = qn_any.shape[:2]
    rows = heads * steps
    pairs = heads // 2
    low, hi = lax.rem(req, 4), lax.div(req, 4)
    bit2 = lax.rem(hi, 2)
    other = 1 - role

    def role_at(rr):
        return role if rr == 0 else other

    def ctx_at(t):
        return lax.rem(ctx + t, n_ctx)

    caches = [pltpu.make_async_copy(cache_ref.at[r], cache_v.at[r], cache_sem.at[r]) for r in range(total)]
    loads = [None,
             pltpu.make_async_copy(wk_ref, wk_v, load_sem.at[1]),
             pltpu.make_async_copy(vu_ref, vu_v, load_sem.at[2]),
             pltpu.make_async_copy(qn_any, qn_ref, load_sem.at[3]),
             pltpu.make_async_copy(qr_any, qr_ref, load_sem.at[4]),
             pltpu.make_async_copy(new_any, new_ref, load_sem.at[5])]
    for one in (3, 4, 5):
        loads[one].start()
    for copy in caches:
        copy.start()

    partners = []
    for d in (1, 2, 3):
        for rr in (0, 1):
            partners.append((role_at(rr), ctx, neighbour(0, d, req)))
    for t in range(n_ctx):
        for rr in (0, 1):
            if t or rr:
                partners.append((role_at(rr), ctx_at(t), req))
    for v in range(1, high):
        far = 4 * lax.rem(hi + v, high)
        for d in (0, 1, 2):
            partners.append((role, ctx, neighbour(0, d, low) + far))
    barrier = pltpu.get_barrier_semaphore()
    for dev in partners:
        pl.semaphore_signal(barrier, inc=1, device_id=dev, device_id_type=MESH)

    started = []

    def send(src, dst, ss, rs, dev):
        copy = pltpu.make_async_remote_copy(src_ref=src, dst_ref=dst, send_sem=ss, recv_sem=rs, device_id=dev,
                                            device_id_type=MESH)
        copy.start()
        started.append(copy)

    def arrived(ref, sem):
        pltpu.make_async_copy(ref, ref, sem).wait()

    def first_row(h):
        return ((h % 2) * pairs + h // 2) * steps

    for one in (3, 4, 5):
        loads[one].wait()
    for slot in range(own):
        for h in range(heads):
            r = first_row(h)
            qn_f[slot, r:r + steps, :] = qn_ref[slot, :, h * nope:(h + 1) * nope].astype(jnp.float32)
        for h in range(pairs):
            qr_f[slot, h * steps:(h + 1) * steps, :] = qr_ref[slot, :, h * 128:(h + 1) * 128].astype(jnp.float32)
        qn_s[slot] = qn_f[slot].astype(jnp.bfloat16)
        qr_s[slot] = qr_f[slot].astype(jnp.bfloat16)
    new_f[...] = jnp.zeros_like(new_f)
    for slot in range(own):
        fresh_rows = new_ref[slot].astype(jnp.float32)
        new_f[slot, :steps, :latent] = fresh_rows[:, :latent]
        new_f[slot, :steps, latent:] = jnp.concatenate([fresh_rows[:, latent:]] * 2, axis=1)

    def request_of(slot):
        def body(j, acc_):
            return jnp.where(slot_ref[j] == slot, j, acc_)
        if total <= 16:
            r = jnp.int32(0)
            for j in range(total):
                r = body(j, r)
            return r
        return lax.fori_loop(0, total, body, jnp.int32(0))

    def k_ref(cl, m, p):
        return k_a.at[m, p] if cl == 0 else k_b.at[(cl - 1) * per + m, p]

    def k_sem(cl, m, p, h):
        return ka_rs.at[m, p, h] if cl == 0 else kb_rs.at[(cl - 1) * per + m, p, h]

    mine_rows = pl.ds(pl.multiple_of(role * half, 16), half)
    order = [(1, 1), (2, 1), (0, 1), (0, 2), (0, 3), (1, 0), (2, 0), (0, 0)]
    todo, lengths = [], {}
    for cl, p in order:
        for to in ((0, 1) if p else (role, other)):
            for m in range(per):
                chip = neighbour(cl, p, req)
                slot = 2 * owner_of(cl, 2 * m + to, chip) + (1 if cl else 0)
                todo.append((cl, p, to, m, chip, request_of(slot)))
    for copy in caches:
        copy.wait()
    loads[1].start()
    loads[2].start()
    pending, delayed = [], []
    cuts = 2 if span % 256 == 0 else 1
    width = span // cuts
    chunk = 0
    for cl, p, to, m, chip, request in todo:
        dst = k_ref(cl, m, p)
        if to is role:
            dst[mine_rows, :] = cache_v[request]
            lengths[cl, m] = len_ref[request]
            continue
        ksend[chunk] = cache_v[request]
        first = m == 0 and cl > 0 and p > 0
        split = first and p > 0 and to == 1
        cut = half // 32 * 16 if split else half
        if cl == 0 and p == 3:
            for c in range(cuts):
                cols = pl.ds(c * width, width)
                delayed.append((ksend.at[chunk, :, cols], dst.at[mine_rows, cols], k_ss.at[chunk, c],
                                k_sem(cl, m, p + c, role), (to, ctx, chip)))
            chunk += 1
            continue
        for begin, end, early in ((0, cut, first), (cut, half, False)):
            if begin < end:
                rows_to = pl.ds(pl.multiple_of(role * half + begin, 16), end - begin)
                (pending if early else delayed).append(
                    (ksend.at[chunk, pl.ds(begin, end - begin)], dst.at[rows_to, :],
                     k_ss.at[chunk, 0 if early else 1], k_sem(cl, m, p, role), (to, ctx, chip)))
        chunk += 1

    kk = jnp.where(bit2 == 0, lax.rem(lax.div(req, 2), 2), lax.rem(req, 2)) + 2 * lax.div(req, 8)
    mine_a, mine_b = (0, hi), (1 + bit2, kk)
    for slot, (cl, k) in ((0, mine_a), (1, mine_b)):
        rawn[cl * two + k] = qn_s[slot]
        rawr[cl * two + k] = qr_s[slot]

    pl.semaphore_wait(barrier, len(partners))

    rcount = [0]

    def share_raw(n_src, r_src, spot, dev):
        n = rcount[0]
        send(n_src, rawn.at[spot], raw_ss.at[n, 0], raw_rs.at[spot, 0], dev)
        send(r_src, rawr.at[spot], raw_ss.at[n, 1], raw_rs.at[spot, 1], dev)
        rcount[0] += 1

    def flipped(chip, bit):
        return jnp.where(bit == 0, xor_bit(chip, 2, 1), xor_bit(chip, 1, 1))

    spot_a, spot_b = hi, (1 + bit2) * two + kk
    for v in range(1, high):
        chip = low + 4 * lax.rem(hi + v, high)
        share_raw(qn_s.at[1], qr_s.at[1], spot_b, (role, ctx, chip))
        share_raw(qn_s.at[0], qr_s.at[0], spot_a, (role, ctx, chip))
    share_raw(qn_s.at[1], qr_s.at[1], spot_b, (role, ctx, flipped(req, bit2)))
    for one in pending:
        send(*one)

    block = BLOCK_HEADS * steps
    half_blocks = pairs // BLOCK_HEADS

    def head_at(hb, j):
        return 2 * (BLOCK_HEADS * lax.rem(hb, half_blocks) + j) + lax.div(hb, half_blocks)

    def absorb(batch):
        shape = (len(batch) * block, BLOCK_HEADS * nope)
        of_row = lax.div(lax.rem(lax.broadcasted_iota(jnp.int32, shape, 0), block), steps)
        of_col = lax.div(lax.broadcasted_iota(jnp.int32, shape, 1), nope)
        diagonal = (of_row == of_col).astype(jnp.float32).astype(jnp.bfloat16)

        def body(hb, carry):
            r0 = pl.multiple_of(hb * block, block)
            lhs = jnp.concatenate([rawn[cl * two + k, pl.ds(r0, block), :] for cl, k in batch], axis=0)
            lhs = jnp.concatenate([lhs] * BLOCK_HEADS, axis=1) * diagonal
            w = jnp.concatenate([wk_v[head_at(hb, j)] for j in range(BLOCK_HEADS)], axis=0)
            res = jnp.dot(lhs, w, preferred_element_type=jnp.float32).astype(jnp.bfloat16)
            for n, (cl, k) in enumerate(batch):
                qa[cl * two + k, pl.ds(r0, block), :] = res[n * block:(n + 1) * block]
            return carry

        lax.fori_loop(0, heads // BLOCK_HEADS, body, 0, unroll=min(UNROLL, heads // BLOCK_HEADS))

    guarded = []
    qcount = [0]

    def share_queries(batch):
        for cl, k in batch:
            e, to = cl * two + k, lax.rem(k, 2)
            sl, rr = cl * per + lax.div(k, 2), lax.rem(to + role, 2)
            for t in list(range(1, n_ctx)) + [0]:
                at = ((n_ctx - t) % n_ctx) * 2 + rr
                n = qcount[0]
                copies = [
                    pltpu.make_async_remote_copy(
                        src_ref=src.at[e], dst_ref=dst.at[sl, at], send_sem=q_ss.at[n, j], recv_sem=q_rs.at[sl, at, j],
                        device_id=(to, ctx_at(t), req), device_id_type=MESH)
                    for j, (src, dst) in ((1, (rawr, r_in)), (0, (qa, q_in)))
                ]
                if t:
                    for copy in copies:
                        copy.start()
                    started.extend(copies)
                else:
                    away = to != role

                    @pl.when(away)
                    def _():
                        for copy in copies:
                            copy.start()
                    guarded.append((away, copies))
                qcount[0] += 1

    def raw_arrived(cl, k):
        arrived(rawn.at[cl * two + k], raw_rs.at[cl * two + k, 0])
        arrived(rawr.at[cl * two + k], raw_rs.at[cl * two + k, 1])

    def class_b(owner):
        bit = lax.rem(lax.div(owner, 4), 2)
        place = jnp.where(bit == 0, lax.rem(lax.div(owner, 2), 2), lax.rem(owner, 2))
        return bit, (1 + bit, place + 2 * lax.div(owner, 8))

    loads[1].wait()
    absorb([mine_b, mine_a])
    share_queries([mine_b, mine_a])
    near, far = [class_b(flipped(req, bit2))[1]], []
    for v in range(1, high):
        owner = low + 4 * lax.rem(hi + v, high)
        bit, entry = class_b(owner)
        raw_arrived(*entry)
        spot = entry[0] * two + entry[1]
        share_raw(rawn.at[spot], rawr.at[spot], spot, (role, ctx, flipped(req, bit)))
        near.append(entry)
        far.append(class_b(flipped(owner, bit))[1])
    for one in delayed:
        send(*one)
    for v in range(1, high):
        entry = (0, lax.rem(hi + v, high))
        raw_arrived(*entry)
        near.append(entry)
    raw_arrived(*near[0])
    absorb(near)
    share_queries(near)
    for entry in far:
        raw_arrived(*entry)
    absorb(far)
    share_queries(far)

    nt = (((1,), (1,)), ((), ()))
    rels = list(range(1, n_ctx)) + [0]
    lane = lax.broadcasted_iota(jnp.int32, (rows // 2, 128), 1)
    even = (lane < 64).astype(jnp.float32).astype(jnp.bfloat16)
    odd = (lane >= 64).astype(jnp.float32).astype(jnp.bfloat16)

    def queries(cl, m, rel):
        sl, k = cl * per + m, cl * two + 2 * m + role
        if rel == 0:
            q_own, r_own = qa[k], rawr[k]
        else:
            q_own, r_own = q_in[sl, rel * 2], r_in[sl, rel * 2]
        r_far = r_in[sl, rel * 2 + 1]
        q = jnp.concatenate([q_own, q_in[sl, rel * 2 + 1]], axis=0)
        qr = jnp.concatenate([r_own * even, r_own * odd, r_far * even, r_far * odd], axis=0)
        return q, qr

    def open_slot(cl, m):
        sl = cl * per + m
        fresh_on = jnp.logical_and(owner_of(cl, 2 * m + role, req) == req, ctx == 0)
        new = new_f[1 if cl else 0].astype(jnp.bfloat16)
        for nth, rel in enumerate(rels):
            for rr in (0, 1):
                if rel or rr:
                    arrived(q_in.at[sl, rel * 2 + rr], q_rs.at[sl, rel * 2 + rr, 0])
                    arrived(r_in.at[sl, rel * 2 + rr], q_rs.at[sl, rel * 2 + rr, 1])
            q, qr = queries(cl, m, rel)
            fresh = (lax.dot_general(q, new[:, :latent], nt, preferred_element_type=jnp.float32)
                     + lax.dot_general(qr, new[:, latent:], nt, preferred_element_type=jnp.float32)) * scale2
            token = lax.broadcasted_iota(jnp.int32, fresh.shape, 1)
            step = lax.rem(lax.broadcasted_iota(jnp.int32, fresh.shape, 0), steps)
            fresh = jnp.where(token <= jnp.where(fresh_on, step, -1), fresh, NEG)
            top = jnp.maximum(jnp.max(fresh, axis=1, keepdims=True), LOW)
            weights = jnp.exp2(fresh - top)
            m_st[nth] = jnp.broadcast_to(top, (2 * rows, 128))
            l_st[nth] = jnp.broadcast_to(jnp.sum(weights, axis=1, keepdims=True), (2 * rows, 128))
            acc[nth] = jnp.dot(weights.astype(jnp.bfloat16), new[:, :latent], preferred_element_type=jnp.float32)

    def await_part(cl, m, p):
        sample = k_ref(cl, m, 0).at[pl.ds(0, half), :]

        @pl.when(p > 0)
        def _():
            arrived(sample, k_sem(cl, m, p, role))
        arrived(sample, k_sem(cl, m, p, other))

    def part(cl, m, p, nth, begin=0, end=2, col=0, wide=None):
        wide = wide or span
        at = slice(begin * rows, end * rows)
        q, qr = queries(cl, m, rels[nth])
        q, qr = q[at], qr[at]
        keys = k_ref(cl, m, p)
        columns = pl.ds(col, wide)
        rotary = keys[latent:, columns]
        s = jnp.dot(q, keys[:latent, columns], preferred_element_type=jnp.float32)
        s += jnp.dot(qr, jnp.concatenate([rotary, rotary], axis=0), preferred_element_type=jnp.float32)
        if cl == 0:
            chip = xor_bit(xor_bit(req, 1, lax.rem(p, 2)), 2, lax.div(p, 2))
        else:
            chip = xor_bit(req, cl, p)
        position = (ctx * n_req + chip) * span + col + lax.broadcasted_iota(jnp.int32, (1, wide), 1)
        s = jnp.where(position < lengths[cl, m], s * scale2, NEG)
        before = m_st[nth, at, :1]
        top = jnp.maximum(before, jnp.max(s, axis=1, keepdims=True))
        keep = jnp.exp2(before - top)
        w = jnp.exp2(s - top)
        m_st[nth, at] = jnp.broadcast_to(top, ((end - begin) * rows, 128))
        l_st[nth, at] = l_st[nth, at] * keep + jnp.sum(w, axis=1, keepdims=True)
        acc[nth, at] = acc[nth, at] * keep + lax.dot_general(w.astype(jnp.bfloat16), keys[:latent, columns], nt,
                                                             preferred_element_type=jnp.float32)

    ocount = [0]

    def close_block(cl, m, nth, pieces=(0, 1)):
        rel = rels[nth]
        sl, k = cl * per + m, cl * two + 2 * m + role
        back = (n_ctx - rel) % n_ctx
        for rr in pieces:
            at = slice(rr * rows, (rr + 1) * rows)
            norm = l_st[nth, at]
            live = norm > 0.0
            safe = jnp.where(live, norm, 1.0)
            piece = (acc[nth, at] * (1.0 / safe[:, :1])).astype(jnp.bfloat16)
            e = jnp.where(live, m_st[nth, at] + jnp.log2(safe), NEG).T[:8]
            if rel == 0 and rr == 0:
                o_in[k, 0] = piece
                e_in[k, 0] = e
                continue
            o_out[sl, rel * 2 + rr] = piece
            e_out[sl, rel * 2 + rr] = e
        for rr in pieces:
            if rel == 0 and rr == 0:
                continue
            dev = (role_at(rr), ctx_at(rel), req)
            n = ocount[0]
            send(e_out.at[sl, rel * 2 + rr], e_in.at[k, back], o_ss.at[n, 1], o_rs.at[k, back, 1], dev)
            send(o_out.at[sl, rel * 2 + rr], o_in.at[k, back], o_ss.at[n, 0], o_rs.at[k, back, 0], dev)
            ocount[0] += 1

    def parts_of(cl, m, first, last):
        def body(p, carry):
            await_part(cl, m, p)
            for nth in range(n_ctx):
                part(cl, m, p, nth)
            return carry
        lax.fori_loop(first, last, body, 0)

    def last_part(cl, m, p):
        p = jnp.int32(p)
        if cl:
            await_part(cl, m, p)
            for nth in range(n_ctx):
                part(cl, m, p, nth)
                close_block(cl, m, nth)
            return
        for c in range(cuts):
            sample = k_ref(cl, m, 0).at[pl.ds(0, half), pl.ds(0, width)]
            arrived(sample, k_sem(cl, m, 3 + c, role))
            arrived(sample, k_sem(cl, m, 3 + c, other))
            for nth in range(n_ctx):
                if c < cuts - 1:
                    part(cl, m, p, nth, 0, 2, c * width, width)
                    continue
                for rr in ((1, 0) if rels[nth] else (0, 1)):
                    part(cl, m, p, nth, rr, rr + 1, c * width, width)
                    close_block(cl, m, nth, (rr,))

    out_rows = lax.broadcasted_iota(jnp.int32, (two * block, 128), 0)
    which = lax.div(lax.rem(out_rows, block), steps)
    def spread(row):
        return jnp.broadcast_to(row[:1], (128, rows)).T

    def merge(cl):
        for rr in (0, 1):
            for m in range(per):
                k = cl * two + 2 * m + role_at(rr)
                for rel in range(n_ctx):
                    if rr or rel:
                        arrived(o_in.at[k, rel], o_rs.at[k, rel, 0])
                        arrived(e_in.at[k, rel], o_rs.at[k, rel, 1])
                es = [e_in[k, rel] for rel in range(n_ctx)]
                top = functools.reduce(jnp.maximum, es)
                shares = [jnp.exp2(e - top) for e in es]
                norm = sum(shares)
                f_out[k] = top + jnp.log2(norm)
                value = 0.0
                for rel in range(n_ctx):
                    w = jnp.concatenate([spread(shares[rel] / norm)] * (latent // 128), axis=1)
                    value = value + o_in[k, rel].astype(jnp.float32) * w
                merged[k] = value.astype(jnp.bfloat16)

        def up(hb, carry):
            r0 = pl.multiple_of(hb * block, block)
            lhs = jnp.concatenate([merged[cl * two + k, pl.ds(r0, block), :] for k in range(two)], axis=0)
            res = jnp.zeros((two * block, 128), jnp.float32)
            for j in range(BLOCK_HEADS):
                one = jnp.dot(lhs, vu_v[head_at(hb, j)], preferred_element_type=jnp.float32)
                res = jnp.where(which == j, one, res)
            res = res.astype(jnp.bfloat16)
            for k in range(two):
                att_out[cl * two + k, pl.ds(r0, block), :] = res[k * block:(k + 1) * block]
            return carry

        lax.fori_loop(0, heads // BLOCK_HEADS, up, 0, unroll=min(UNROLL, heads // BLOCK_HEADS))
        for k in range(two):
            e = cl * two + k
            owner = owner_of(cl, jnp.int32(k), req)
            if cl == 0:
                at, dst, fdst, sems = hi, att_a, f_a, ta_rs
            elif cl == 1:
                at, dst, fdst, sems = lax.div(req, 2), att_b, f_b, tb_rs
            else:
                at, dst, fdst, sems = lax.rem(req, 2) + 2 * hi, att_b, f_b, tb_rs
            copies = [
                pltpu.make_async_remote_copy(
                    src_ref=src.at[e], dst_ref=d.at[at], send_sem=t_ss.at[e, j], recv_sem=sems.at[at, j],
                    device_id=(role, ctx, owner), device_id_type=MESH)
                for j, (src, d) in enumerate(((att_out, dst), (f_out, fdst)))
            ]

            @pl.when(owner != req)
            def _():
                for copy in copies:
                    copy.start()

            @pl.when(owner == req)
            def _():
                dst[at] = att_out[e]
                fdst[at] = f_out[e]
            guarded.append((owner != req, copies))

    own_b = jnp.where(bit2 == 0, lax.div(req, 2), lax.rem(req, 2) + 2 * hi)

    def combine(slot):
        count, src, fsrc, sems, mine = ((high, att_a, f_a, ta_rs, hi), (4 * per, att_b, f_b, tb_rs, own_b))[slot]
        for j in range(count):
            @pl.when(mine != j)
            def _():
                arrived(src.at[j], sems.at[j, 0])
                arrived(fsrc.at[j], sems.at[j, 1])
        es = [fsrc[j] for j in range(count)]
        top = functools.reduce(jnp.maximum, es)
        shares = [jnp.exp2(e - top) for e in es]
        norm = sum(shares)
        value = 0.0
        for j in range(count):
            value = value + src[j].astype(jnp.float32) * spread(shares[j] / norm)
        fin[slot] = value
        for h in range(heads):
            r = first_row(h)
            out_ref[slot, :, h * 128:(h + 1) * 128] = fin[slot, r:r + steps, :].astype(jnp.bfloat16)

    for cl in (1, 2):
        for m in range(per):
            open_slot(cl, m)
            parts_of(cl, m, 0, 1)
            last_part(cl, m, 1)
    for m in range(per):
        open_slot(0, m)
        parts_of(0, m, 0, 3)
        if m == per - 1:
            loads[2].wait()
            merge(1)
            merge(2)
        last_part(0, m, 3)
    combine(1)
    merge(0)
    combine(0)

    for copy in started:
        copy.wait_send()
    for sent, copies in guarded:
        @pl.when(sent)
        def _():
            for copy in copies:
                copy.wait_send()


def shards(cache, lengths, request_decode_slot, q_nope, q_rope, new_latent, w_key, value_up_weight):
    total = request_decode_slot.shape[0]
    n_req, n_ctx = lax.axis_size("req"), lax.axis_size("ctx")
    heads, nope, latent = w_key.shape
    vdim = value_up_weight.shape[2]
    own, steps = q_nope.shape[:2]
    rope = q_rope.shape[2] // heads
    span, half = cache.shape[1:]
    rows = heads * steps
    per, two, high = n_req // 8, n_req // 4, n_req // 4
    groups = 2 * n_ctx
    scale2 = (nope + rope) ** (-0.5) * math.log2(math.e)

    turned = jnp.swapaxes(cache, 1, 2)
    bf, f32 = jnp.bfloat16, jnp.float32
    chunks = total - 3 * per
    vm, dma = pltpu.VMEM, pltpu.SemaphoreType.DMA
    smem = pl.BlockSpec(memory_space=pltpu.SMEM)
    away = pl.BlockSpec(memory_space=pl.ANY)
    out = pl.pallas_call(
        functools.partial(kernel, (n_req, n_ctx, scale2)),
        out_shape=pltpu.VMEM((own, steps, heads * vdim), bf),
        in_specs=[smem, smem, away, away, away, away, away, away],
        out_specs=pl.BlockSpec(memory_space=pltpu.VMEM),
        scratch_shapes=[
            vm(q_nope.shape, bf),
            vm(q_rope.shape, bf),
            vm(new_latent.shape, bf),
            vm((total, half, span), bf),
            vm((chunks, half, span), bf),
            vm((per, 4, 2 * half, span), bf),
            vm((2 * per, 2, 2 * half, span), bf),
            vm(w_key.shape, bf),
            vm(value_up_weight.shape, bf),
            vm((own, rows, nope), f32),
            vm((own, rows // 2, 2 * rope), f32),
            vm((own, rows, nope), bf),
            vm((own, rows // 2, 2 * rope), bf),
            vm((own, 128, latent + 2 * rope), f32),
            vm((3 * two, rows, nope), bf),
            vm((3 * two, rows // 2, 2 * rope), bf),
            vm((3 * two, rows, latent), bf),
            vm((3 * per, groups, rows, latent), bf),
            vm((3 * per, groups, rows // 2, 2 * rope), bf),
            vm((n_ctx, 2 * rows, 128), f32),
            vm((n_ctx, 2 * rows, 128), f32),
            vm((n_ctx, 2 * rows, latent), f32),
            vm((3 * per, groups, rows, latent), bf),
            vm((3 * per, groups, 8, rows), f32),
            vm((3 * two, n_ctx, rows, latent), bf),
            vm((3 * two, n_ctx, 8, rows), f32),
            vm((3 * two, rows, latent), bf),
            vm((3 * two, rows, vdim), bf),
            vm((3 * two, 8, rows), f32),
            vm((high, rows, vdim), bf),
            vm((high, 8, rows), f32),
            vm((4 * per, rows, vdim), bf),
            vm((4 * per, 8, rows), f32),
            vm((own, rows, vdim), f32),
            dma((6 + own,)),
            dma((total,)),
            dma((3 * high, 2)),
            dma((3 * two, 2)),
            dma((chunks, 2)),
            dma((per, 5, 2)),
            dma((2 * per, 2, 2)),
            dma((3 * two * n_ctx, 2)),
            dma((3 * per, groups, 2)),
            dma((3 * per * (groups - 1), 2)),
            dma((3 * two, n_ctx, 2)),
            dma((3 * two, 2)),
            dma((high, 2)),
            dma((4 * per, 2)),
        ],
        compiler_params=pltpu.CompilerParams(
            collective_id=0, has_side_effects=True, vmem_limit_bytes=62 * 1024 * 1024
        ),
    )(request_decode_slot, lengths, turned, q_nope, q_rope, new_latent, w_key, value_up_weight)
    return out


def solution(mesh):
    placed = (
        P(None, ("ctx", "req"), "role"),
        P(),
        P(),
        P("req", None, ("role", "ctx")),
        P("req", None, ("role", "ctx")),
        P("req", None, None),
        P(("role", "ctx"), None, None),
        P(("role", "ctx"), None, None),
    )
    return jax.shard_map(
        shards,
        mesh=mesh,
        in_specs=placed,
        out_specs=P("req", None, ("role", "ctx")),
        check_vma=False,
    )
```
